256 devices in a mesh: tok: 64 (over x, z, core), head: 4 (over y).
Axes of the slice: x: 4, y: 4, z: 8, core: 2. Of those that a mesh axis runs over, the one named last changes fastest.
Arguments:
- head_inputs: bfloat16 [32768, 2048], P('tok', 'head'), may hold values from -6 to 6
- state_keys: bfloat16 [32768, 128], P('tok'), may hold values from -2 to 2
- state_queries: bfloat16 [32768, 128], P('tok'), may hold values from -2 to 2
- log_decay: float32 [32768, 32], P('tok', 'head'), may hold values from -1.6 to 0, as said below
- level_weight: float32 [32768, 32, 18], P('tok', 'head'), may hold values from 0.2 to 2
- skip_scale: float32 [32], P('head'), may hold values from 0.5 to 2
- gate_input: bfloat16 [32768, 2048], P('tok', 'head'), may hold values from -500 to 500
- norm_gain: float32 [2048], P('head'), may hold values from 0.5 to 1.5
Outputs:
- mixer_out: bfloat16 [32768, 2048], P('tok', 'head')
The draws below stay inside these ranges and needn't reach their ends.
Inputs may be any that keep to these rules, and one draw needn't show every extreme that they name: `log_decay`: every entry is negative.
All inputs are finite; a program needn't handle non-finite values.
Results may differ from the reference program's by a relative error of at most 0.0038.
Values sent between devices are 32-bit elements; how exact they have to be, the bound alone decides.
No kernel may reach another device: no remote copies, remote signals or barrier semaphores. Data moves between devices by JAX's collectives and lax.ppermute only.
A program may use at most 64 MiB of HBM per device.

```python
import math
import jax
import jax.numpy as jnp
import numpy as np
from jax import lax

HEAD_TOTAL = 32
HEAD_DIM = 64
STATE_DIM = 128
TOK_DEV = 512
LEVELS = 18
TOKEN_TOTAL = 32768


def draw_log_decay(key, part):
    sequence_flows = jax.random.split(key, 7)
    slow_share = 0.5
    slow_heads = jax.random.uniform(sequence_flows[0], (HEAD_TOTAL,), jnp.float32) < slow_share
    fast_rate = jnp.exp(jax.random.uniform(sequence_flows[1], (HEAD_TOTAL,), jnp.float32, math.log(1.0 / 110.0), math.log(1.0 / 100.0)))
    slow_rate = jnp.exp(jax.random.uniform(sequence_flows[2], (HEAD_TOTAL,), jnp.float32, math.log(0.1), 0.0)) * math.log(10.0) / (8.0 * TOKEN_TOTAL)
    rate = jnp.where(slow_heads, slow_rate, fast_rate)
    roughness = jax.random.uniform(sequence_flows[3], (TOKEN_TOTAL, HEAD_TOTAL), jnp.float32, 0.5, 1.5)
    block_factor = jax.random.uniform(sequence_flows[4], (TOKEN_TOTAL // TOK_DEV, HEAD_TOTAL), jnp.float32, 1.0, 1.2)
    block_factor = jnp.repeat(block_factor, TOK_DEV, axis=0)
    baseline_level = -rate[None, :] * roughness * block_factor
    spike_location = jax.random.randint(sequence_flows[5], (2,), 0, TOKEN_TOTAL)
    spike_value = jnp.log(jax.random.uniform(sequence_flows[6], (2, HEAD_TOTAL), jnp.float32, 0.5, 0.8))
    spike_flagged = (jnp.arange(TOKEN_TOTAL, dtype=jnp.int32)[:, None] == spike_location[None, :]).astype(jnp.float32)
    return (baseline_level + jnp.dot(spike_flagged, spike_value)).astype(jnp.float32)


def draw_gate_input(key, part):
    sequence_flows = jax.random.split(key, 3)
    columns = HEAD_TOTAL * HEAD_DIM
    column_scale = jnp.exp(math.log(3.0) * jnp.arange(columns, dtype=jnp.float32) / columns + jax.random.uniform(sequence_flows[0], (columns,), jnp.float32, 0.0, math.log(10.0)))
    row_scale = jnp.exp(jax.random.uniform(sequence_flows[1], (TOKEN_TOTAL, 1), jnp.float32, 0.0, math.log(4.0)))
    base_draw = jnp.clip(jax.random.normal(sequence_flows[2], (TOKEN_TOTAL, columns), jnp.float32), -4.0, 4.0)
    return (base_draw * row_scale * column_scale[None, :]).astype(jnp.bfloat16)


def steps_of(stream_key, extent, cuts, low, largest):
    gain, own = 1.0, jax.random.fold_in(stream_key, 6)
    for position, blocks in cuts:
        steps = jnp.exp(jax.random.uniform(jax.random.fold_in(own, position), (blocks,), jnp.float32, low / len(cuts), largest / len(cuts)))
        gain = gain * jnp.repeat(steps, extent[position] // blocks).reshape([-1 if axis == position else 1 for axis in range(len(extent))])
    return gain


def scatter_about(key, extent, deviation, most, cuts=(), kind=jnp.bfloat16):
    values = jax.random.normal(key, extent, jnp.float32) * deviation
    if len(cuts) > 0:
        values = steps_of(key, extent, cuts, -0.22, 0.18) * values
    return jnp.clip(values, min=-most, max=most).astype(kind)


def setup_inputs(seed: int = 0) -> dict:
    key_of = jax.random.split(jax.random.key(seed), 9)
    head_inputs = scatter_about(key_of[0], (TOKEN_TOTAL, HEAD_TOTAL * HEAD_DIM), 1.0, 6.0, ((0, 64), (1, 4)))
    state_keys = scatter_about(key_of[1], (TOKEN_TOTAL, STATE_DIM), 0.3, 2.0, ((0, 64),))
    state_queries = scatter_about(key_of[2], (TOKEN_TOTAL, STATE_DIM), 0.3, 2.0, ((0, 64),))
    log_decay = draw_log_decay(jax.random.fold_in(key_of[8], 71), 0)
    level_weight = jnp.clip(jnp.exp(math.log(2.0) - 2.3025851 * jax.random.uniform(key_of[4], (TOKEN_TOTAL, HEAD_TOTAL, LEVELS), jnp.float32) ** steps_of(key_of[4], (TOKEN_TOTAL, HEAD_TOTAL, LEVELS), ((0, 64), (1, 4)), -0.2, 0.2)), 0.2, 2.0)
    skip_scale = jnp.clip(0.5 + 1.5 * jax.random.uniform(key_of[5], (HEAD_TOTAL,), jnp.float32) ** steps_of(key_of[5], (HEAD_TOTAL,), ((0, 4),), -0.2, 0.2), 0.5, 2.0)
    gate_input = draw_gate_input(jax.random.fold_in(key_of[8], 71), 0)
    norm_gain = jnp.clip(0.5 + 1.0 * jax.random.uniform(key_of[7], (HEAD_TOTAL * HEAD_DIM,), jnp.float32) ** steps_of(key_of[7], (HEAD_TOTAL * HEAD_DIM,), ((0, 4),), -0.2, 0.2), 0.5, 1.5)
    return dict(head_inputs=head_inputs, state_keys=state_keys, state_queries=state_queries, log_decay=log_decay, level_weight=level_weight, skip_scale=skip_scale, gate_input=gate_input, norm_gain=norm_gain)


def block_levels(first_row, row_count, col_count, local_bits):
    query_pos = first_row + jnp.arange(row_count, dtype=jnp.int32)
    key_pos = jnp.arange(col_count, dtype=jnp.int32)
    crossing = jnp.bitwise_xor(query_pos[:, None], key_pos[None, :])
    level_map = jnp.zeros((row_count, col_count), jnp.int32)
    for shift_bit in range(local_bits):
        level_map = level_map + (crossing >= 1 << shift_bit).astype(jnp.int32)
    return (level_map, key_pos[None, :] <= query_pos[:, None])

def local_mix(queries, key_rows, values, decays, scales, local_bits):
    block_len = queries.shape[0]
    row_block = min(512, block_len)
    pieces_out = []
    for first_row in range(0, block_len, row_block):
        last_row = first_row + row_block
        scores = jnp.dot(queries[first_row:last_row], key_rows[:last_row].T, preferred_element_type=jnp.float32)
        level_map, causal = block_levels(first_row, row_block, last_row, local_bits)

        def one_head(inputs):
            decay_row, scale_row, value_row = inputs
            spread = jnp.where(causal, decay_row[first_row:last_row, None] - decay_row[None, :last_row], -jnp.inf)
            chosen = jnp.zeros((row_block, last_row), jnp.float32)
            for level_index in range(local_bits + 1):
                chosen = chosen + jnp.where(level_map == level_index, scale_row[first_row:last_row, level_index:level_index + 1], 0.0)
            weighted = (scores * jnp.exp(spread) * chosen).astype(jnp.bfloat16)
            return jnp.dot(weighted, value_row[:last_row], preferred_element_type=jnp.float32)
        pieces_out.append(lax.map(one_head, (decays, scales, values)))
    return jnp.concatenate(pieces_out, axis=1)

def make_state(key_rows, values, decays):
    scaled = (key_rows.astype(jnp.float32)[None] * jnp.exp(decays[:, -1:] - decays)[:, :, None]).astype(jnp.bfloat16)
    return jnp.einsum('htn,htp->hnp', scaled.astype(jnp.float32), values.astype(jnp.float32), precision=lax.Precision.HIGHEST)

def far_mix(queries, decays, scales, crossed, first_level):
    query_wide = queries.astype(jnp.float32)
    tree_bits = crossed.shape[1]

    def one_head(inputs):
        decay_row, scale_row, state_row = inputs
        stacked = state_row.transpose(1, 0, 2).reshape(state_row.shape[1], -1)
        readout = jnp.dot(query_wide, stacked, precision=lax.Precision.HIGHEST).reshape(query_wide.shape[0], tree_bits, -1)
        level_scale = scale_row[:, first_level:first_level + tree_bits]
        return jnp.exp(decay_row)[:, None] * lax.optimization_barrier(jnp.sum(level_scale[:, :, None] * readout, axis=1))
    return lax.map(one_head, (decays, scales, crossed))

def head_mix(queries, key_rows, values, decays, scales, crossed, gates, skip_scale, local_bits):
    nearby = local_mix(queries, key_rows, values, decays, scales, local_bits)
    distant = far_mix(queries, decays, scales, crossed, local_bits + 1)
    mixed_out = nearby + distant + skip_scale[:, None, None] * values.astype(jnp.float32)
    head_count, block_len, head_size = mixed_out.shape
    mixed_out = mixed_out.transpose(1, 0, 2).reshape(block_len, head_count * head_size)
    return mixed_out * jax.nn.silu(gates.astype(jnp.float32))

def reference(head_inputs, state_keys, state_queries, log_decay, level_weight, skip_scale, gate_input, norm_gain):
    block_count = TOKEN_TOTAL // TOK_DEV
    local_bits = TOK_DEV.bit_length() - 1
    tree_bits = block_count.bit_length() - 1
    head_values = head_inputs.reshape(block_count, TOK_DEV, HEAD_TOTAL, HEAD_DIM).transpose(0, 2, 1, 3)
    decay_sum = jnp.cumsum(log_decay.reshape(block_count, TOK_DEV, HEAD_TOTAL), axis=1).transpose(0, 2, 1)
    weights = level_weight.reshape(block_count, TOK_DEV, HEAD_TOTAL, LEVELS).transpose(0, 2, 1, 3)
    key_blocks = state_keys.reshape(block_count, TOK_DEV, STATE_DIM)
    query_blocks = state_queries.reshape(block_count, TOK_DEV, STATE_DIM)
    gate_blocks = gate_input.reshape(block_count, TOK_DEV, HEAD_TOTAL * HEAD_DIM)

    def state_block(inputs):
        return make_state(inputs[0], inputs[1], inputs[2])
    states = lax.map(state_block, (key_blocks, head_values, decay_sum))
    totals = decay_sum[:, :, -1]
    collected = []
    for level_bit in range(tree_bits):
        group_size = 1 << level_bit
        group_totals = totals.reshape(block_count // group_size, group_size, HEAD_TOTAL)
        after_sum = jnp.cumsum(group_totals[:, ::-1], axis=1)[:, ::-1] - group_totals
        before_sum = jnp.cumsum(group_totals, axis=1) - group_totals
        group_states = states.reshape(block_count // group_size, group_size, HEAD_TOTAL, STATE_DIM, HEAD_DIM)
        merged = lax.optimization_barrier(jnp.sum(group_states * jnp.exp(after_sum)[:, :, :, None, None], axis=1))
        group_index = np.arange(block_count) // group_size
        upper_half = group_index % 2 == 1
        sibling = np.maximum(group_index - 1, 0)
        picked = merged[sibling] * jnp.exp(before_sum.reshape(block_count, HEAD_TOTAL))[:, :, None, None]
        collected.append(jnp.where(jnp.asarray(upper_half)[:, None, None, None], picked, 0.0))
    crossed = jnp.stack(collected, axis=2)

    def one_block(inputs):
        queries, key_rows, values, decays, scales, states_here, gates = inputs
        gated_out = head_mix(queries, key_rows, values, decays, scales, states_here, gates, skip_scale, local_bits)
        squares = lax.optimization_barrier(jnp.mean(gated_out * gated_out, axis=1, keepdims=True))
        return (gated_out * lax.rsqrt(squares + 1e-05) * norm_gain).astype(jnp.bfloat16)
    result = lax.map(one_block, (query_blocks, key_blocks, head_values, decay_sum, weights, crossed, gate_blocks))
    return result.reshape(TOKEN_TOTAL, HEAD_TOTAL * HEAD_DIM)
```

```python
import functools

import jax
import jax.numpy as jnp
from jax import lax
from jax.experimental import pallas as pl
from jax.experimental.pallas import tpu as pltpu
from jax.sharding import PartitionSpec as P

epsilon = 1e-05
BLOCK = 512
HEADS = 8
WIDTH = 64
STATE = 128
CHUNKS = 2
CHUNK_HEADS = HEADS // 2 // CHUNKS
CHUNK_ROWS = CHUNK_HEADS * WIDTH
BUF_ROWS = CHUNK_ROWS + HEADS
LOCAL_BITS = 9
TREE_BITS = 6
F32 = jnp.float32
BF16 = jnp.bfloat16
VM = pl.BlockSpec(memory_space=pltpu.VMEM)
SM = pl.BlockSpec(memory_space=pltpu.SMEM)
MIB = 1024 * 1024


def call(body, outs, ins, name, flops, aliases=None, scratch=(), vmem=12):
    return pl.pallas_call(
        body,
        out_shape=outs,
        in_specs=ins,
        out_specs=jax.tree.map(lambda _: VM, outs),
        scratch_shapes=list(scratch),
        input_output_aliases=aliases or {},
        name=name,
        cost_estimate=pl.CostEstimate(flops=flops, bytes_accessed=MIB, transcendentals=0),
        compiler_params=pltpu.CompilerParams(vmem_limit_bytes=vmem * MIB),
    )


def sds(shape, dtype=F32):
    return jax.ShapeDtypeStruct(shape, dtype)


def core_index():
    return lax.axis_index("tok") & 1


def split3(x):
    hi = x.astype(BF16).astype(F32)
    rest = x - hi
    mid = rest.astype(BF16).astype(F32)
    return hi, mid, rest - mid


def prep_body(ld_ref, v_ref, k_ref, d_ref, dcol_ref, vt_ref, *rest):
    own_refs, send_refs, state_ref = rest[:CHUNKS], rest[CHUNKS : 2 * CHUNKS], rest[-1]
    core = core_index()
    ld = ld_ref[...]
    parts = jnp.concatenate([*split3(ld), jnp.zeros_like(ld)], axis=0).astype(BF16)
    row = lax.broadcasted_iota(jnp.int32, (BLOCK, BLOCK), 0)
    col = lax.broadcasted_iota(jnp.int32, (BLOCK, BLOCK), 1)
    upto = (row <= col).astype(F32).astype(BF16)
    sums = jnp.dot(parts, upto, preferred_element_type=F32)
    d = sums[0:8] + sums[8:16] + sums[16:24]
    d_ref[...] = d
    total = jnp.broadcast_to(d[:, BLOCK - 1 : BLOCK], (HEADS, BLOCK))
    toend = jnp.exp(total - d)
    vt = v_ref[...].T
    vt_ref[...] = vt
    scaled = [
        (vt[h * WIDTH : (h + 1) * WIDTH].astype(F32) * toend[h : h + 1]).astype(BF16)
        for h in range(HEADS)
    ]
    state_ref[...] = jnp.dot(
        jnp.concatenate(scaled, axis=0), k_ref[...], preferred_element_type=F32
    )
    for k in range(CHUNKS):
        mine = pl.multiple_of(core * (HEADS // 2 * WIDTH) + k * CHUNK_ROWS, CHUNK_ROWS)
        other = pl.multiple_of((1 - core) * (HEADS // 2 * WIDTH) + k * CHUNK_ROWS, CHUNK_ROWS)
        own_refs[k][0:CHUNK_ROWS] = state_ref[pl.ds(mine, CHUNK_ROWS), :]
        own_refs[k][CHUNK_ROWS:BUF_ROWS] = total[:, 0:STATE]
        send_refs[k][0:CHUNK_ROWS] = state_ref[pl.ds(other, CHUNK_ROWS), :]
        send_refs[k][CHUNK_ROWS:BUF_ROWS] = total[:, 0:STATE]
    dcol_ref[...] = d.T


def prep(ld, v, k):
    buf = sds((BUF_ROWS, STATE))
    outs = [sds((HEADS, BLOCK)), sds((BLOCK, HEADS)), sds((BLOCK, BLOCK), BF16)]
    outs += [buf] * (2 * CHUNKS)
    got = call(
        prep_body, outs, [VM] * 3, "prep", 10**9,
        scratch=[pltpu.VMEM((HEADS * WIDTH, STATE), F32)],
    )(ld, v, k)
    return got[0], got[1], got[2], got[3 : 3 + CHUNKS], got[3 + CHUNKS :]


def merge_body(level, chunk, own_ref, got_ref, out_ref, fac_ref):
    upper = ((lax.axis_index("tok") >> level) & 1) == 1
    own_ext = own_ref[CHUNK_ROWS:BUF_ROWS]
    got_ext = got_ref[CHUNK_ROWS:BUF_ROWS]
    one = jnp.ones_like(own_ext)
    fac_ref[0:HEADS] = jnp.where(upper, one, jnp.exp(got_ext))
    fac_ref[HEADS : 2 * HEADS] = jnp.where(upper, jnp.exp(own_ext), one)
    first = core_index() * (HEADS // 2) + chunk * CHUNK_HEADS
    for j in range(CHUNK_HEADS):
        rows = slice(j * WIDTH, (j + 1) * WIDTH)
        fa = fac_ref[pl.ds(first + j, 1), :]
        fb = fac_ref[pl.ds(first + (HEADS + j), 1), :]
        out_ref[rows] = own_ref[rows] * fa + got_ref[rows] * fb
    out_ref[CHUNK_ROWS:BUF_ROWS] = own_ext + got_ext


def merge(level, chunk, own, got):
    return call(
        functools.partial(merge_body, level, chunk), sds((BUF_ROWS, STATE)), [VM] * 2,
        "merge", 10**7, scratch=[pltpu.VMEM((2 * HEADS, STATE), F32)], vmem=4,
    )(own, got)


def aux_body(q_ref, gate_ref, qt_ref, gt_ref):
    qt = q_ref[...].T
    qt_ref[0:STATE] = qt
    qt_ref[STATE : 2 * STATE] = qt
    for j in range(4):
        cols = slice(j * 128, (j + 1) * 128)
        v = gate_ref[:, cols].T.astype(F32)
        gt_ref[cols] = v / (1.0 + jnp.exp(-v))


def aux(q, gate):
    return call(
        aux_body, [sds((2 * STATE, BLOCK), BF16), sds((BLOCK, BLOCK))], [VM] * 2, "aux", 10**9
    )(q, gate)


def near_body(first, k_ref, qt_ref, vt_ref, d_ref, dcol_ref, w_ref, skip_ref, out_ref, sc_ref, mix_ref):
    sc_ref[...] = jnp.dot(k_ref[...], qt_ref[0:STATE], preferred_element_type=F32)
    half = BLOCK // 2
    mix_ref[half:BLOCK, 0:half] = jnp.zeros((half, half), BF16)
    mix_ref[128:256, 0:128] = jnp.zeros((128, 128), BF16)
    mix_ref[384:512, 256:384] = jnp.zeros((128, 128), BF16)
    srow = lax.broadcasted_iota(jnp.int32, (128, 128), 0)
    tcol = lax.broadcasted_iota(jnp.int32, (128, 128), 1)
    cross = srow ^ tcol
    causal = srow <= tcol
    for n in range(2):
        h = first + n
        for i in range(4):
            rows = slice(i * 128, (i + 1) * 128)
            dcol = jnp.broadcast_to(dcol_ref[rows, h : h + 1], (128, 128))
            for j in range(i, 4):
                cols = slice(j * 128, (j + 1) * 128)
                spread = d_ref[h : h + 1, cols] - dcol
                if i == j:
                    spread = jnp.where(causal, spread, -jnp.inf)
                    chosen = jnp.broadcast_to(w_ref[0, h : h + 1, cols], (128, 128))
                    for level in range(1, 8):
                        chosen = jnp.where(
                            cross >= 1 << (level - 1), w_ref[level, h : h + 1, cols], chosen
                        )
                else:
                    chosen = w_ref[7 + (i ^ j).bit_length(), h : h + 1, cols]
                mix_ref[rows, cols] = (sc_ref[rows, cols] * jnp.exp(spread) * chosen).astype(BF16)
        mine = slice(h * WIDTH, (h + 1) * WIDTH)
        here = slice(n * WIDTH, (n + 1) * WIDTH)
        vt = vt_ref[mine]
        skip = vt.astype(F32) * skip_ref[h]
        out_ref[here, 0:half] = skip[:, 0:half] + jnp.dot(
            vt[:, 0:half], mix_ref[0:half, 0:half], preferred_element_type=F32
        )
        out_ref[here, half:BLOCK] = skip[:, half:BLOCK] + jnp.dot(
            vt, mix_ref[:, half:BLOCK], preferred_element_type=F32
        )


def near(first, k, qt, vt, d, dcol, w, skip):
    return call(
        functools.partial(near_body, first), sds((2 * WIDTH, BLOCK)), [VM] * 6 + [SM],
        f"near{first}", 10**9,
        scratch=[pltpu.VMEM((BLOCK, BLOCK), F32), pltpu.VMEM((BLOCK, BLOCK), BF16)],
    )(k, qt, vt, d, dcol, w, skip)


def readout(level, acc_rows, emit, qt_ref, d_ref, w_ref, lead_ref, buf_refs, coef_ref):
    upper = ((lax.axis_index("tok") >> level) & 1) == 1
    lead = lead_ref[...]
    gain = jnp.where(upper, jnp.exp(lead), 0.0)[:, 0:1]
    coef_ref[...] = w_ref[LOCAL_BITS + 1 + level] * jnp.exp(d_ref[...]) * gain
    core = core_index()
    for side in range(2):
        base = (core if side == 0 else 1 - core) * (HEADS // 2)
        for k in range(CHUNKS):
            states = buf_refs[side * CHUNKS + k][0:CHUNK_ROWS]
            hi = states.astype(BF16)
            lo = (states - hi.astype(F32)).astype(BF16)
            read = jnp.dot(
                jnp.concatenate([hi, lo], axis=1), qt_ref[...], preferred_element_type=F32
            )
            for j in range(CHUNK_HEADS):
                head = base + (k * CHUNK_HEADS + j)
                row = pl.multiple_of(head * WIDTH, WIDTH)
                term = read[j * WIDTH : (j + 1) * WIDTH] * coef_ref[pl.ds(head, 1), :]
                emit(row, acc_rows(row) + term)
    got = buf_refs[0][CHUNK_ROWS:BUF_ROWS]
    return lead + jnp.where(upper, got, 0.0)


def far_body(level, qt_ref, d_ref, w_ref, lead_ref, acc_ref, *rest):
    bufs, out_ref, next_ref, coef_ref = rest[: 2 * CHUNKS], rest[-3], rest[-2], rest[-1]

    def emit(row, value):
        out_ref[pl.ds(row, WIDTH), :] = value

    next_ref[...] = readout(
        level, lambda row: acc_ref[pl.ds(row, WIDTH), :], emit,
        qt_ref, d_ref, w_ref, lead_ref, bufs, coef_ref,
    )


def far(level, qt, d, w, lead, acc, bufs):
    return call(
        functools.partial(far_body, level), [sds((BLOCK, BLOCK)), sds((HEADS, STATE))],
        [VM] * (5 + 2 * CHUNKS), f"far{level}", 10**9, aliases={4: 0},
        scratch=[pltpu.VMEM((HEADS, BLOCK), F32)],
    )(qt, d, w, lead, acc, *bufs)


def close_body(level, qt_ref, d_ref, w_ref, lead_ref, acc_ref, gt_ref, *rest):
    bufs, out_ref, sq_ref, coef_ref = rest[: 2 * CHUNKS], rest[-3], rest[-2], rest[-1]
    sums = []

    def emit(row, value):
        gated = value * gt_ref[pl.ds(row, WIDTH), :]
        out_ref[pl.ds(row, WIDTH), :] = gated
        sums.append(jnp.sum(gated * gated, axis=0, keepdims=True))

    readout(
        level, lambda row: acc_ref[pl.ds(row, WIDTH), :], emit,
        qt_ref, d_ref, w_ref, lead_ref, bufs, coef_ref,
    )
    sq_ref[...] = sum(sums[1:], sums[0])


def close(level, qt, d, w, lead, acc, gt, bufs):
    return call(
        functools.partial(close_body, level), [sds((BLOCK, BLOCK)), sds((1, BLOCK))],
        [VM] * (6 + 2 * CHUNKS), "close", 10**9,
        scratch=[pltpu.VMEM((HEADS, BLOCK), F32)],
    )(qt, d, w, lead, acc, gt, *bufs)


def turn_body(g_ref, gain_ref, out_ref):
    for j in range(4):
        rows = slice(j * 128, (j + 1) * 128)
        out_ref[rows] = g_ref[:, rows].T * gain_ref[...]


def turn(g, gain):
    return call(turn_body, sds((BLOCK, BLOCK)), [VM] * 2, "turn", 10**8)(g, gain)


def finish_body(width, g_ref, a_ref, b_ref, c_ref, e_ref, out_ref):
    total = a_ref[...] + b_ref[...] + c_ref[...] + e_ref[...]
    scale = lax.rsqrt(total / width + epsilon)
    column = jnp.broadcast_to(scale, (8, BLOCK)).T[:, 0:1]
    out_ref[...] = (g_ref[...] * column).astype(BF16)


def finish(width, g, sums):
    return call(
        functools.partial(finish_body, width), sds((BLOCK, BLOCK), BF16), [VM] * 5, "finish", 10**8
    )(g, *sums)


def route_of(partner):
    return [(i, partner(i)) for i in range(1 << TREE_BITS)]


def partner_of(level):
    flip = (1, 2, 6, 14, 16, 48)[level]
    return route_of(lambda i: i ^ flip)


def shards(head_inputs, state_keys, state_queries, log_decay, level_weight, skip_scale, gate_input, norm_gain):
    w = level_weight.transpose(2, 1, 0)
    d, dcol, vt, own, send = prep(log_decay.T, head_inputs, state_keys)
    swap = lambda x: lax.ppermute(x, "tok", partner_of(0))
    got = [swap(x) for x in send]
    other = [swap(x) for x in own]
    qt, gt = aux(state_queries, gate_input)
    levels = [(got, other)]
    sums = [merge(0, k, own[k], got[k]) for k in range(CHUNKS)]
    for level in range(1, TREE_BITS):
        got = [lax.ppermute(x, "tok", partner_of(level)) for x in sums]
        if level + 1 < TREE_BITS:
            sums = [merge(level, k, sums[k], got[k]) for k in range(CHUNKS)]
        levels.append((got, [swap(x) for x in got]))
    acc = jnp.concatenate(
        [near(h, state_keys, qt, vt, d, dcol, w, skip_scale) for h in range(0, HEADS, 2)], axis=0
    )
    lead = jnp.zeros((HEADS, STATE), F32)
    for level in range(TREE_BITS - 1):
        acc, lead = far(level, qt, d, w, lead, acc, (*levels[level][0], *levels[level][1]))
    last = TREE_BITS - 1
    gated, squares = close(last, qt, d, w, lead, acc, gt, (*levels[last][0], *levels[last][1]))
    count = lax.axis_size("head")
    shares = [
        lax.ppermute(squares, "head", [(i, (i + s) % count) for i in range(count)])
        for s in range(1, count)
    ]
    turned = turn(gated, norm_gain[None])
    return finish(HEADS * WIDTH * count, turned, [squares, *shares])


def solution(mesh):
    return jax.shard_map(
        shards,
        mesh=mesh,
        in_specs=(
            P("tok", "head"),
            P("tok", None),
            P("tok", None),
            P("tok", "head"),
            P("tok", "head", None),
            P("head"),
            P("tok", "head"),
            P("head"),
        ),
        out_specs=P("tok", "head"),
        check_vma=False,
    )
```

```python
import functools

import jax
import jax.numpy as jnp
from jax import lax
from jax.experimental import pallas as pl
from jax.experimental.pallas import tpu as pltpu
from jax.sharding import PartitionSpec as P

epsilon = 1e-05
BLOCK = 512
HEADS = 8
WIDTH = 64
STATE = 128
CHUNKS = 1
CHUNK_HEADS = HEADS // 2 // CHUNKS
CHUNK_ROWS = CHUNK_HEADS * WIDTH
BUF_ROWS = CHUNK_ROWS + HEADS
LOCAL_BITS = 9
TREE_BITS = 6
F32 = jnp.float32
BF16 = jnp.bfloat16
VM = pl.BlockSpec(memory_space=pltpu.VMEM)
SM = pl.BlockSpec(memory_space=pltpu.SMEM)
HB = pl.BlockSpec(memory_space=pltpu.HBM)
MIB = 1024 * 1024


def call(body, outs, ins, name, flops, aliases=None, scratch=(), vmem=12, out_space=VM):
    return pl.pallas_call(
        body,
        out_shape=outs,
        in_specs=ins,
        out_specs=jax.tree.map(lambda _: out_space, outs),
        scratch_shapes=list(scratch),
        input_output_aliases=aliases or {},
        name=name,
        cost_estimate=pl.CostEstimate(flops=flops, bytes_accessed=MIB, transcendentals=0),
        compiler_params=pltpu.CompilerParams(vmem_limit_bytes=vmem * MIB),
    )


def sds(shape, dtype=F32):
    return jax.ShapeDtypeStruct(shape, dtype)


def core_index():
    return lax.axis_index("tok") & 1


def split3(x):
    hi = x.astype(BF16).astype(F32)
    rest = x - hi
    mid = rest.astype(BF16).astype(F32)
    return hi, mid, rest - mid


def prep_body(ld_hbm, v_hbm, k_hbm, d_ref, dcol_ref, vt_ref, *rest):
    own_refs, send_refs = rest[:CHUNKS], rest[CHUNKS : 2 * CHUNKS]
    state_ref, ld_ref, v_ref, k_ref, sems = rest[2 * CHUNKS :]
    pairs = ((ld_hbm, ld_ref), (v_hbm, v_ref), (k_hbm, k_ref))
    copies = [pltpu.make_async_copy(a, b, sems.at[i]) for i, (a, b) in enumerate(pairs)]
    for copy in copies:
        copy.start()
    core = core_index()
    copies[0].wait()
    ld = ld_ref[...]
    parts = jnp.concatenate([*split3(ld), jnp.zeros_like(ld)], axis=0).astype(BF16)
    row = lax.broadcasted_iota(jnp.int32, (BLOCK, BLOCK), 0)
    col = lax.broadcasted_iota(jnp.int32, (BLOCK, BLOCK), 1)
    upto = (row <= col).astype(F32).astype(BF16)
    sums = jnp.dot(parts, upto, preferred_element_type=F32)
    d = sums[0:8] + sums[8:16] + sums[16:24]
    d_ref[...] = d
    total = jnp.broadcast_to(d[:, BLOCK - 1 : BLOCK], (HEADS, BLOCK))
    toend = jnp.exp(total - d)
    copies[1].wait()
    vt = v_ref[...].T
    vt_ref[...] = vt
    scaled = [
        (vt[h * WIDTH : (h + 1) * WIDTH].astype(F32) * toend[h : h + 1]).astype(BF16)
        for h in range(HEADS)
    ]
    copies[2].wait()
    state_ref[...] = jnp.dot(
        jnp.concatenate(scaled, axis=0), k_ref[...], preferred_element_type=F32
    )
    for k in range(CHUNKS):
        mine = pl.multiple_of(core * (HEADS // 2 * WIDTH) + k * CHUNK_ROWS, CHUNK_ROWS)
        other = pl.multiple_of((1 - core) * (HEADS // 2 * WIDTH) + k * CHUNK_ROWS, CHUNK_ROWS)
        own_refs[k][0:CHUNK_ROWS] = state_ref[pl.ds(mine, CHUNK_ROWS), :]
        own_refs[k][CHUNK_ROWS:BUF_ROWS] = total[:, 0:STATE]
        send_refs[k][0:CHUNK_ROWS] = state_ref[pl.ds(other, CHUNK_ROWS), :]
        send_refs[k][CHUNK_ROWS:BUF_ROWS] = total[:, 0:STATE]
    dcol_ref[...] = d.T


def prep(ld, v, k):
    buf = sds((BUF_ROWS, STATE))
    outs = [sds((HEADS, BLOCK)), sds((BLOCK, HEADS)), sds((BLOCK, BLOCK), BF16)]
    outs += [buf] * (2 * CHUNKS)
    got = call(
        prep_body, outs, [HB] * 3, "prep", 10**9,
        scratch=[
            pltpu.VMEM((HEADS * WIDTH, STATE), F32),
            pltpu.VMEM((HEADS, BLOCK), F32),
            pltpu.VMEM((BLOCK, HEADS * WIDTH), BF16),
            pltpu.VMEM((BLOCK, STATE), BF16),
            pltpu.SemaphoreType.DMA((3,)),
        ],
    )(*(pltpu.with_memory_space_constraint(x, pltpu.HBM) for x in (ld, v, k)))
    return got[0], got[1], got[2], got[3 : 3 + CHUNKS], got[3 + CHUNKS :]


def merge_body(level, chunk, own_ref, got_ref, out_ref, fac_ref):
    upper = ((lax.axis_index("tok") >> level) & 1) == 1
    own_ext = own_ref[CHUNK_ROWS:BUF_ROWS]
    got_ext = got_ref[CHUNK_ROWS:BUF_ROWS]
    one = jnp.ones_like(own_ext)
    fac_ref[0:HEADS] = jnp.where(upper, one, jnp.exp(got_ext))
    fac_ref[HEADS : 2 * HEADS] = jnp.where(upper, jnp.exp(own_ext), one)
    first = core_index() * (HEADS // 2) + chunk * CHUNK_HEADS
    for j in range(CHUNK_HEADS):
        rows = slice(j * WIDTH, (j + 1) * WIDTH)
        fa = fac_ref[pl.ds(first + j, 1), :]
        fb = fac_ref[pl.ds(first + (HEADS + j), 1), :]
        out_ref[rows] = own_ref[rows] * fa + got_ref[rows] * fb
    out_ref[CHUNK_ROWS:BUF_ROWS] = own_ext + got_ext


def merge(level, chunk, own, got):
    return call(
        functools.partial(merge_body, level, chunk), sds((BUF_ROWS, STATE)), [VM] * 2,
        "merge", 10**7, scratch=[pltpu.VMEM((2 * HEADS, STATE), F32)], vmem=4,
    )(own, got)


def aux_body(q_ref, gate_ref, qt_ref, gt_ref):
    qt = q_ref[...].T
    qt_ref[0:STATE] = qt
    qt_ref[STATE : 2 * STATE] = qt
    for j in range(4):
        cols = slice(j * 128, (j + 1) * 128)
        v = gate_ref[:, cols].T.astype(F32)
        gt_ref[cols] = v / (1.0 + jnp.exp(-v))


def aux(q, gate):
    return call(
        aux_body, [sds((2 * STATE, BLOCK), BF16), sds((BLOCK, BLOCK))], [VM] * 2, "aux", 10**9
    )(q, gate)


def near_body(first, k_ref, qt_ref, vt_ref, d_ref, dcol_ref, w_ref, skip_ref, token_ref, out_ref, sc_ref, mix_ref):
    sc_ref[...] = jnp.dot(k_ref[...], qt_ref[0:STATE], preferred_element_type=F32)
    half = BLOCK // 2
    mix_ref[half:BLOCK, 0:half] = jnp.zeros((half, half), BF16)
    mix_ref[128:256, 0:128] = jnp.zeros((128, 128), BF16)
    mix_ref[384:512, 256:384] = jnp.zeros((128, 128), BF16)
    srow = lax.broadcasted_iota(jnp.int32, (128, 128), 0)
    tcol = lax.broadcasted_iota(jnp.int32, (128, 128), 1)
    cross = srow ^ tcol
    causal = srow <= tcol
    for n in range(2):
        h = first + n
        for i in range(4):
            rows = slice(i * 128, (i + 1) * 128)
            dcol = jnp.broadcast_to(dcol_ref[rows, h : h + 1], (128, 128))
            for j in range(i, 4):
                cols = slice(j * 128, (j + 1) * 128)
                spread = d_ref[h : h + 1, cols] - dcol
                if i == j:
                    spread = jnp.where(causal, spread, -jnp.inf)
                    chosen = jnp.broadcast_to(w_ref[0, h : h + 1, cols], (128, 128))
                    for level in range(1, 8):
                        chosen = jnp.where(
                            cross >= 1 << (level - 1), w_ref[level, h : h + 1, cols], chosen
                        )
                else:
                    chosen = w_ref[7 + (i ^ j).bit_length(), h : h + 1, cols]
                mix_ref[rows, cols] = (sc_ref[rows, cols] * jnp.exp(spread) * chosen).astype(BF16)
        mine = slice(h * WIDTH, (h + 1) * WIDTH)
        here = slice(n * WIDTH, (n + 1) * WIDTH)
        vt = vt_ref[mine]
        skip = vt.astype(F32) * skip_ref[h]
        out_ref[here, 0:half] = skip[:, 0:half] + jnp.dot(
            vt[:, 0:half], mix_ref[0:half, 0:half], preferred_element_type=F32
        )
        out_ref[here, half:BLOCK] = skip[:, half:BLOCK] + jnp.dot(
            vt, mix_ref[:, half:BLOCK], preferred_element_type=F32
        )


def near(first, k, qt, vt, d, dcol, w, skip, token):
    return call(
        functools.partial(near_body, first), sds((2 * WIDTH, BLOCK)), [VM] * 6 + [SM, VM],
        f"near{first}", 10**9,
        scratch=[pltpu.VMEM((BLOCK, BLOCK), F32), pltpu.VMEM((BLOCK, BLOCK), BF16)],
    )(k, qt, vt, d, dcol, w, skip, token)


def readout(level, acc_rows, emit, qt_ref, d_ref, w_ref, lead_ref, buf_refs, coef_ref):
    upper = ((lax.axis_index("tok") >> level) & 1) == 1
    lead = lead_ref[...]
    gain = jnp.where(upper, jnp.exp(lead), 0.0)[:, 0:1]
    coef_ref[...] = w_ref[LOCAL_BITS + 1 + level] * jnp.exp(d_ref[...]) * gain
    core = core_index()
    for side in range(2):
        base = (core if side == 0 else 1 - core) * (HEADS // 2)
        for k in range(CHUNKS):
            states = buf_refs[side * CHUNKS + k][0:CHUNK_ROWS]
            hi = states.astype(BF16)
            lo = (states - hi.astype(F32)).astype(BF16)
            read = jnp.dot(
                jnp.concatenate([hi, lo], axis=1), qt_ref[...], preferred_element_type=F32
            )
            for j in range(CHUNK_HEADS):
                head = base + (k * CHUNK_HEADS + j)
                row = pl.multiple_of(head * WIDTH, WIDTH)
                term = read[j * WIDTH : (j + 1) * WIDTH] * coef_ref[pl.ds(head, 1), :]
                emit(row, acc_rows(row) + term)
    got = buf_refs[0][CHUNK_ROWS:BUF_ROWS]
    return lead + jnp.where(upper, got, 0.0)


def far_body(level, qt_ref, d_ref, w_ref, lead_ref, *rest):
    coef_ref, next_ref, out_ref = rest[-1], rest[-2], rest[-3]
    bufs = rest[: 2 * CHUNKS]

    def emit(row, value):
        out_ref[pl.ds(row, WIDTH), :] = value

    def start(row):
        return rest[2 * CHUNKS][pl.ds(row, WIDTH), :] if level > 0 else 0.0

    next_ref[...] = readout(level, start, emit, qt_ref, d_ref, w_ref, lead_ref, bufs, coef_ref)
    if level > 0:
        rows = slice((level - 1) * 2 * WIDTH, level * 2 * WIDTH)
        out_ref[rows] = out_ref[rows] + rest[2 * CHUNKS + 1][...]


def far(level, qt, d, w, lead, bufs, *more):
    return call(
        functools.partial(far_body, level), [sds((BLOCK, BLOCK)), sds((HEADS, STATE))],
        [VM] * (4 + 2 * CHUNKS + len(more)), f"far{level}", 10**9,
        aliases={4 + 2 * CHUNKS: 0} if more else None,
        scratch=[pltpu.VMEM((HEADS, BLOCK), F32)],
    )(qt, d, w, lead, *bufs, *more)


def close_body(level, qt_ref, d_ref, w_ref, lead_ref, acc_ref, gt_ref, *rest):
    bufs, out_ref, sq_ref, coef_ref = rest[: 2 * CHUNKS], rest[-3], rest[-2], rest[-1]
    sums = []

    def emit(row, value):
        gated = value * gt_ref[pl.ds(row, WIDTH), :]
        out_ref[pl.ds(row, WIDTH), :] = gated
        sums.append(jnp.sum(gated * gated, axis=0, keepdims=True))

    readout(
        level, lambda row: acc_ref[pl.ds(row, WIDTH), :], emit,
        qt_ref, d_ref, w_ref, lead_ref, bufs, coef_ref,
    )
    sq_ref[...] = sum(sums[1:], sums[0])


def close(level, qt, d, w, lead, acc, gt, bufs):
    return call(
        functools.partial(close_body, level), [sds((BLOCK, BLOCK)), sds((1, BLOCK))],
        [VM] * (6 + 2 * CHUNKS), "close", 10**9,
        scratch=[pltpu.VMEM((HEADS, BLOCK), F32)],
    )(qt, d, w, lead, acc, gt, *bufs)


def turn_body(g_ref, gain_ref, out_ref):
    for j in range(4):
        rows = slice(j * 128, (j + 1) * 128)
        out_ref[rows] = g_ref[:, rows].T * gain_ref[...]


def turn(g, gain):
    return call(turn_body, sds((BLOCK, BLOCK)), [VM] * 2, "turn", 10**8)(g, gain)


def finish_body(width, g_ref, a_ref, b_ref, c_ref, e_ref, out_hbm, out_ref, sems):
    total = a_ref[...] + b_ref[...] + c_ref[...] + e_ref[...]
    scale = lax.rsqrt(total / width + epsilon)
    copies = []
    for j in range(4):
        rows = slice(j * 128, (j + 1) * 128)
        column = jnp.broadcast_to(scale[:, rows], (128, 128)).T
        for i in range(4):
            cols = slice(i * 128, (i + 1) * 128)
            out_ref[rows, cols] = (g_ref[rows, cols] * column).astype(BF16)
        copies.append(pltpu.make_async_copy(out_ref.at[rows], out_hbm.at[rows], sems.at[j]))
        copies[-1].start()
    for copy in copies:
        copy.wait()


def finish(width, g, sums):
    return call(
        functools.partial(finish_body, width), sds((BLOCK, BLOCK), BF16), [VM] * 5, "finish",
        10**8, out_space=HB,
        scratch=[pltpu.VMEM((BLOCK, BLOCK), BF16), pltpu.SemaphoreType.DMA((4,))],
    )(g, *sums)


def route_of(partner):
    return [(i, partner(i)) for i in range(1 << TREE_BITS)]


def partner_of(level):
    flip = (1, 2, 6, 14, 16, 48)[level]
    return route_of(lambda i: i ^ flip)


def shards(head_inputs, state_keys, state_queries, log_decay, level_weight, skip_scale, gate_input, norm_gain):
    w = level_weight.transpose(2, 1, 0)
    d, dcol, vt, own, send = prep(log_decay.T, head_inputs, state_keys)
    swap = lambda x: lax.ppermute(x, "tok", partner_of(0))
    got = [swap(x) for x in send]
    other = [swap(x) for x in own]
    qt, gt = aux(state_queries, gate_input)
    levels = [(got, other)]
    sums = [merge(0, k, own[k], got[k]) for k in range(CHUNKS)]
    parts = []
    for level in range(1, TREE_BITS):
        if level < 5:
            parts.append(
                near(2 * (level - 1), state_keys, qt, vt, d, dcol, w, skip_scale, sums[-1])
            )
        got = [lax.ppermute(x, "tok", partner_of(level)) for x in sums]
        if level + 1 < TREE_BITS:
            sums = [merge(level, k, sums[k], got[k]) for k in range(CHUNKS)]
        levels.append((got, [swap(x) for x in got]))
    lead = jnp.zeros((HEADS, STATE), F32)
    acc, lead = far(0, qt, d, w, lead, (*levels[0][0], *levels[0][1]))
    for level in range(1, TREE_BITS - 1):
        bufs = (*levels[level][0], *levels[level][1])
        acc, lead = far(level, qt, d, w, lead, bufs, acc, parts[level - 1])
    last = TREE_BITS - 1
    gated, squares = close(last, qt, d, w, lead, acc, gt, (*levels[last][0], *levels[last][1]))
    count = lax.axis_size("head")
    shares = [
        lax.ppermute(squares, "head", [(i, (i + s) % count) for i in range(count)])
        for s in range(1, count)
    ]
    turned = turn(gated, norm_gain[None])
    return finish(HEADS * WIDTH * count, turned, [squares, *shares])


def solution(mesh):
    return jax.shard_map(
        shards,
        mesh=mesh,
        in_specs=(
            P("tok", "head"),
            P("tok", None),
            P("tok", None),
            P("tok", "head"),
            P("tok", "head", None),
            P("head"),
            P("tok", "head"),
            P("head"),
        ),
        out_specs=P("tok", "head"),
        check_vma=False,
    )
```

```python
import functools

import jax
import jax.numpy as jnp
from jax import lax
from jax.experimental import pallas as pl
from jax.experimental.pallas import tpu as pltpu
from jax.sharding import PartitionSpec as P


epsilon = 1e-05
BLOCK = 512
HEADS = 8
WIDTH = 64
STATE = 128
CHUNKS = 2
CHUNK_HEADS = HEADS // 2 // CHUNKS
CHUNK_ROWS = CHUNK_HEADS * WIDTH
BUF_ROWS = CHUNK_ROWS + HEADS
HALF_ROWS = CHUNKS * CHUNK_ROWS
LOCAL_BITS = 9
TREE_BITS = 6
F32 = jnp.float32
BF16 = jnp.bfloat16
VM = pl.BlockSpec(memory_space=pltpu.VMEM)
SM = pl.BlockSpec(memory_space=pltpu.SMEM)
HB = pl.BlockSpec(memory_space=pltpu.HBM)
MIB = 1024 * 1024


def call(body, outs, ins, flops, aliases=None, scratch=(), vmem=12, out_space=VM):
    return pl.pallas_call(
        body,
        out_shape=outs,
        in_specs=ins,
        out_specs=jax.tree.map(lambda _: out_space, outs),
        scratch_shapes=list(scratch),
        input_output_aliases=aliases or {},
        cost_estimate=pl.CostEstimate(flops=flops, bytes_accessed=MIB, transcendentals=0),
        compiler_params=pltpu.CompilerParams(vmem_limit_bytes=vmem * MIB),
    )


def sds(shape, dtype=F32):
    return jax.ShapeDtypeStruct(shape, dtype)


def core_index():
    return lax.axis_index("tok") & 1


def split3(x):
    hi = x.astype(BF16).astype(F32)
    rest = x - hi
    mid = rest.astype(BF16).astype(F32)
    return hi, mid, rest - mid


def prep_body(ld_hbm, v_hbm, k_hbm, d_ref, dcol_ref, vt_ref, *rest):
    own_refs, send_refs = rest[:CHUNKS], rest[CHUNKS : 2 * CHUNKS]
    pack_ref, state_ref, ld_ref, v_ref, k_ref, sems = rest[2 * CHUNKS :]
    pairs = ((ld_hbm, ld_ref), (v_hbm, v_ref), (k_hbm, k_ref))
    copies = [pltpu.make_async_copy(a, b, sems.at[i]) for i, (a, b) in enumerate(pairs)]
    for copy in copies:
        copy.start()
    core = core_index()
    copies[0].wait()
    ld = ld_ref[...]
    parts = jnp.concatenate([*split3(ld), jnp.zeros_like(ld)], axis=0).astype(BF16)
    row = lax.broadcasted_iota(jnp.int32, (BLOCK, BLOCK), 0)
    col = lax.broadcasted_iota(jnp.int32, (BLOCK, BLOCK), 1)
    upto = (row <= col).astype(F32).astype(BF16)
    sums = jnp.dot(parts, upto, preferred_element_type=F32)
    d = sums[0:8] + sums[8:16] + sums[16:24]
    d_ref[...] = d
    total = jnp.broadcast_to(d[:, BLOCK - 1 : BLOCK], (HEADS, BLOCK))
    toend = jnp.exp(total - d)
    copies[1].wait()
    vt = v_ref[...].T
    vt_ref[...] = vt
    scaled = [
        (vt[h * WIDTH : (h + 1) * WIDTH].astype(F32) * toend[h : h + 1]).astype(BF16)
        for h in range(HEADS)
    ]
    copies[2].wait()
    state_ref[...] = jnp.dot(
        jnp.concatenate(scaled, axis=0), k_ref[...], preferred_element_type=F32
    )
    for k in range(CHUNKS):
        mine = pl.multiple_of(core * (HEADS // 2 * WIDTH) + k * CHUNK_ROWS, CHUNK_ROWS)
        other = pl.multiple_of((1 - core) * (HEADS // 2 * WIDTH) + k * CHUNK_ROWS, CHUNK_ROWS)
        own_refs[k][0:CHUNK_ROWS] = state_ref[pl.ds(mine, CHUNK_ROWS), :]
        own_refs[k][CHUNK_ROWS:BUF_ROWS] = total[:, 0:STATE]
        send_refs[k][0:CHUNK_ROWS] = state_ref[pl.ds(other, CHUNK_ROWS), :]
        send_refs[k][CHUNK_ROWS:BUF_ROWS] = total[:, 0:STATE]
    pack_ref[...] = state_ref[pl.ds(pl.multiple_of(core * HALF_ROWS, HALF_ROWS), HALF_ROWS), :]
    dcol_ref[...] = d.T


def prep(ld, v, k):
    buf = sds((BUF_ROWS, STATE))
    outs = [sds((HEADS, BLOCK)), sds((BLOCK, HEADS)), sds((BLOCK, BLOCK), BF16)]
    outs += [buf] * (2 * CHUNKS) + [sds((HALF_ROWS, STATE))]
    got = call(
        prep_body, outs, [HB] * 3, 10**7,
        scratch=[
            pltpu.VMEM((HEADS * WIDTH, STATE), F32),
            pltpu.VMEM((HEADS, BLOCK), F32),
            pltpu.VMEM((BLOCK, HEADS * WIDTH), BF16),
            pltpu.VMEM((BLOCK, STATE), BF16),
            pltpu.SemaphoreType.DMA((3,)),
        ],
    )(*(pltpu.with_memory_space_constraint(x, pltpu.HBM) for x in (ld, v, k)))
    return got[0], got[1], got[2], got[3 : 3 + CHUNKS], got[3 + CHUNKS : -1], got[-1]


def merge_body(level, chunk, own_ref, got_ref, *refs):
    out_ref, fac_ref = refs[-2:]
    upper = ((lax.axis_index("tok") >> level) & 1) == 1
    own_ext = own_ref[CHUNK_ROWS:BUF_ROWS]
    got_ext = got_ref[CHUNK_ROWS:BUF_ROWS]
    one = jnp.ones_like(own_ext)
    fac_ref[0:HEADS] = jnp.where(upper, one, jnp.exp(got_ext))
    fac_ref[HEADS : 2 * HEADS] = jnp.where(upper, jnp.exp(own_ext), one)
    first = core_index() * (HEADS // 2) + chunk * CHUNK_HEADS
    for j in range(CHUNK_HEADS):
        rows = slice(j * WIDTH, (j + 1) * WIDTH)
        fa = fac_ref[pl.ds(first + j, 1), :]
        fb = fac_ref[pl.ds(first + (HEADS + j), 1), :]
        out_ref[rows] = own_ref[rows] * fa + got_ref[rows] * fb
    out_ref[CHUNK_ROWS:BUF_ROWS] = own_ext + got_ext


def merge(level, chunk, own, got, tokens):
    return call(
        functools.partial(merge_body, level, chunk), sds((BUF_ROWS, STATE)),
        [VM] * (2 + len(tokens)), 10**5,
        scratch=[pltpu.VMEM((2 * HEADS, STATE), F32)], vmem=4,
    )(own, got, *tokens)


def merge_all(level, own, got, tokens):
    out = []
    for k in range(CHUNKS):
        out.append(merge(level, k, own[k], got[k], tokens))
        tokens = out[-1:]
    return out


def pack_body(*refs):
    for k, ref in enumerate(refs[:CHUNKS]):
        refs[-1][k * CHUNK_ROWS : (k + 1) * CHUNK_ROWS] = ref[0:CHUNK_ROWS]


def pack(got, token):
    return call(pack_body, sds((HALF_ROWS, STATE)), [VM] * (CHUNKS + 1), 10**5, vmem=4)(*got, token)


def aux_body(q_ref, gate_ref, qt_ref, gt_ref):
    qt = q_ref[...].T
    qt_ref[0:STATE] = qt
    qt_ref[STATE : 2 * STATE] = qt
    for j in range(4):
        cols = slice(j * 128, (j + 1) * 128)
        v = gate_ref[:, cols].T.astype(F32)
        gt_ref[cols] = v / (1.0 + jnp.exp(-v))


def aux(q, gate):
    return call(
        aux_body, [sds((2 * STATE, BLOCK), BF16), sds((BLOCK, BLOCK))], [VM] * 2, 10**7
    )(q, gate)


def near_body(first, k_ref, qt_ref, vt_ref, d_ref, dcol_ref, w_ref, skip_ref, token_ref, out_ref, sc_ref, mix_ref):
    sc_ref[...] = jnp.dot(k_ref[...], qt_ref[0:STATE], preferred_element_type=F32)
    half = BLOCK // 2
    mix_ref[half:BLOCK, 0:half] = jnp.zeros((half, half), BF16)
    mix_ref[128:256, 0:128] = jnp.zeros((128, 128), BF16)
    mix_ref[384:512, 256:384] = jnp.zeros((128, 128), BF16)
    srow = lax.broadcasted_iota(jnp.int32, (128, 128), 0)
    tcol = lax.broadcasted_iota(jnp.int32, (128, 128), 1)
    cross = srow ^ tcol
    causal = srow <= tcol
    for n in range(2):
        h = first + n
        for i in range(4):
            rows = slice(i * 128, (i + 1) * 128)
            dcol = jnp.broadcast_to(dcol_ref[rows, h : h + 1], (128, 128))
            for j in range(i, 4):
                cols = slice(j * 128, (j + 1) * 128)
                spread = d_ref[h : h + 1, cols] - dcol
                if i == j:
                    spread = jnp.where(causal, spread, -jnp.inf)
                    chosen = jnp.broadcast_to(w_ref[0, h : h + 1, cols], (128, 128))
                    for level in range(1, 8):
                        chosen = jnp.where(
                            cross >= 1 << (level - 1), w_ref[level, h : h + 1, cols], chosen
                        )
                else:
                    chosen = w_ref[7 + (i ^ j).bit_length(), h : h + 1, cols]
                mix_ref[rows, cols] = (sc_ref[rows, cols] * jnp.exp(spread) * chosen).astype(BF16)
        mine = slice(h * WIDTH, (h + 1) * WIDTH)
        here = slice(n * WIDTH, (n + 1) * WIDTH)
        vt = vt_ref[mine]
        skip = vt.astype(F32) * skip_ref[h]
        out_ref[here, 0:half] = skip[:, 0:half] + jnp.dot(
            vt[:, 0:half], mix_ref[0:half, 0:half], preferred_element_type=F32
        )
        out_ref[here, half:BLOCK] = skip[:, half:BLOCK] + jnp.dot(
            vt, mix_ref[:, half:BLOCK], preferred_element_type=F32
        )


def near(first, k, qt, vt, d, dcol, w, skip, token):
    return call(
        functools.partial(near_body, first), sds((2 * WIDTH, BLOCK)), [VM] * 6 + [SM, VM],
        10**7,
        scratch=[pltpu.VMEM((BLOCK, BLOCK), F32), pltpu.VMEM((BLOCK, BLOCK), BF16)],
    )(k, qt, vt, d, dcol, w, skip, token)


def readout(level, acc_rows, emit, qt_ref, d_ref, w_ref, lead_ref, buf_refs, coef_ref):
    upper = ((lax.axis_index("tok") >> level) & 1) == 1
    lead = lead_ref[...]
    gain = jnp.where(upper, jnp.exp(lead), 0.0)[:, 0:1]
    coef_ref[...] = w_ref[LOCAL_BITS + 1 + level] * jnp.exp(d_ref[...]) * gain
    core = core_index()
    places = [(core, k * CHUNK_HEADS, CHUNK_HEADS) for k in range(CHUNKS)]
    if len(buf_refs) == 2 * CHUNKS:
        places += [(1 - core, k * CHUNK_HEADS, CHUNK_HEADS) for k in range(CHUNKS)]
    else:
        places += [(1 - core, 0, HEADS // 2)]
    for ref, (side, first, heads) in zip(buf_refs, places):
        states = ref[0 : heads * WIDTH]
        hi = states.astype(BF16)
        lo = (states - hi.astype(F32)).astype(BF16)
        read = jnp.dot(jnp.concatenate([hi, lo], axis=1), qt_ref[...], preferred_element_type=F32)
        for j in range(heads):
            head = side * (HEADS // 2) + (first + j)
            row = pl.multiple_of(head * WIDTH, WIDTH)
            term = read[j * WIDTH : (j + 1) * WIDTH] * coef_ref[pl.ds(head, 1), :]
            emit(row, acc_rows(row) + term)
    got = buf_refs[0][CHUNK_ROWS:BUF_ROWS]
    return lead + jnp.where(upper, got, 0.0)


def far_body(level, qt_ref, d_ref, w_ref, lead_ref, *rest):
    coef_ref, next_ref, out_ref = rest[-1], rest[-2], rest[-3]
    bufs = rest[: CHUNKS + 1]

    def emit(row, value):
        out_ref[pl.ds(row, WIDTH), :] = value

    def start(row):
        return rest[CHUNKS + 1][pl.ds(row, WIDTH), :] if level > 0 else 0.0

    next_ref[...] = readout(level, start, emit, qt_ref, d_ref, w_ref, lead_ref, bufs, coef_ref)
    if level > 0:
        rows = slice((level - 1) * 2 * WIDTH, level * 2 * WIDTH)
        out_ref[rows] = out_ref[rows] + rest[CHUNKS + 2][...]


def far(level, qt, d, w, lead, bufs, *more):
    return call(
        functools.partial(far_body, level), [sds((BLOCK, BLOCK)), sds((HEADS, STATE))],
        [VM] * (5 + CHUNKS + len(more)), 10**7,
        aliases={5 + CHUNKS: 0} if more else None,
        scratch=[pltpu.VMEM((HEADS, BLOCK), F32)],
    )(qt, d, w, lead, *bufs, *more)


def close_body(level, qt_ref, d_ref, w_ref, lead_ref, acc_ref, gt_ref, *rest):
    bufs, out_ref, sq_ref, coef_ref = rest[: 2 * CHUNKS], rest[-3], rest[-2], rest[-1]
    sums = []

    def emit(row, value):
        gated = value * gt_ref[pl.ds(row, WIDTH), :]
        out_ref[pl.ds(row, WIDTH), :] = gated
        sums.append(jnp.sum(gated * gated, axis=0, keepdims=True))

    readout(
        level, lambda row: acc_ref[pl.ds(row, WIDTH), :], emit,
        qt_ref, d_ref, w_ref, lead_ref, bufs, coef_ref,
    )
    sq_ref[...] = sum(sums[1:], sums[0])


def close(level, qt, d, w, lead, acc, gt, bufs):
    return call(
        functools.partial(close_body, level), [sds((BLOCK, BLOCK)), sds((1, BLOCK))],
        [VM] * (6 + 2 * CHUNKS), 10**7,
        scratch=[pltpu.VMEM((HEADS, BLOCK), F32)],
    )(qt, d, w, lead, acc, gt, *bufs)


def turn_body(g_ref, gain_ref, out_ref):
    for j in range(4):
        rows = slice(j * 128, (j + 1) * 128)
        out_ref[rows] = g_ref[:, rows].T * gain_ref[...]


def turn(g, gain):
    return call(turn_body, sds((BLOCK, BLOCK)), [VM] * 2, 10**7)(g, gain)


def finish_body(width, g_ref, a_ref, b_ref, c_ref, e_ref, out_hbm, out_ref, sems):
    total = a_ref[...] + b_ref[...] + c_ref[...] + e_ref[...]
    scale = lax.rsqrt(total / width + epsilon)
    copies = []
    for j in range(4):
        rows = slice(j * 128, (j + 1) * 128)
        column = jnp.broadcast_to(scale[:, rows], (128, 128)).T
        for i in range(4):
            cols = slice(i * 128, (i + 1) * 128)
            out_ref[rows, cols] = (g_ref[rows, cols] * column).astype(BF16)
        copies.append(pltpu.make_async_copy(out_ref.at[rows], out_hbm.at[rows], sems.at[j]))
        copies[-1].start()
    for copy in copies:
        copy.wait()


def finish(width, g, sums):
    return call(
        functools.partial(finish_body, width), sds((BLOCK, BLOCK), BF16), [VM] * 5,
        10**8, out_space=HB,
        scratch=[pltpu.VMEM((BLOCK, BLOCK), BF16), pltpu.SemaphoreType.DMA((4,))],
    )(g, *sums)


def route_of(partner):
    return [(i, partner(i)) for i in range(1 << TREE_BITS)]


def partner_of(level):
    flip = (1, 2, 6, 14, 16, 48)[level]
    return route_of(lambda i: i ^ flip)


def work(head_inputs, state_keys, state_queries, log_decay, level_weight, skip_scale, gate_input, norm_gain):
    w = level_weight.transpose(2, 1, 0)
    d, dcol, vt, own, send, packed = prep(log_decay.T, head_inputs, state_keys)
    swap = lambda x: lax.ppermute(x, "tok", partner_of(0))
    got = [swap(x) for x in send]
    qt, gt = aux(state_queries, gate_input)
    sums = merge_all(0, own, got, [gt])
    levels = [(*got, swap(packed))]
    acc, lead = None, jnp.zeros((HEADS, STATE), F32)
    parts = []
    for level in range(1, TREE_BITS):
        before = []
        if level < 5:
            first = 2 * (level - 1)
            parts.append(near(first, state_keys, qt, vt, d, dcol, w, skip_scale, sums[-1]))
            before.append(parts[-1])
        if level > 1:
            more = () if acc is None else (acc, parts[level - 3])
            acc, lead = far(level - 2, qt, d, w, lead, levels[level - 2], *more)
            before.append(acc)
        got = []
        for x in sums:
            got.append(lax.ppermute(x, "tok", partner_of(level)))
        if level + 1 < TREE_BITS:
            sums = merge_all(level, sums, got, before)
            levels.append((*got, swap(pack(got, sums[-1]))))
        else:
            levels.append((*got, *[swap(x) for x in got]))
    acc, lead = far(TREE_BITS - 2, qt, d, w, lead, levels[TREE_BITS - 2], acc, parts[-1])
    last = TREE_BITS - 1
    gated, squares = close(last, qt, d, w, lead, acc, gt, levels[last])
    count = lax.axis_size("head")
    shares = [
        lax.ppermute(squares, "head", [(i, (i + s) % count) for i in range(count)])
        for s in range(1, count)
    ]
    turned = turn(gated, norm_gain[None])
    return finish(HEADS * WIDTH * count, turned, [squares, *shares])


def solution(mesh):
    return jax.shard_map(
        work,
        mesh=mesh,
        in_specs=(
            P("tok", "head"),
            P("tok", None),
            P("tok", None),
            P("tok", "head"),
            P("tok", "head", None),
            P("head"),
            P("tok", "head"),
            P("head"),
        ),
        out_specs=P("tok", "head"),
        check_vma=False,
    )
```

```python
import functools

import jax
import jax.numpy as jnp
from jax import lax
from jax.experimental import pallas as pl
from jax.experimental.pallas import tpu as pltpu
from jax.sharding import PartitionSpec as P


epsilon = 1e-05
BLOCK = 512
HEADS = 8
WIDTH = 64
STATE = 128
HALF = HEADS // 2
ROWS = HALF * WIDTH
BUF_ROWS = ROWS + HEADS
LOCAL_BITS = 9
F32 = jnp.float32
BF16 = jnp.bfloat16
VM = pl.BlockSpec(memory_space=pltpu.VMEM)
SM = pl.BlockSpec(memory_space=pltpu.SMEM)
HB = pl.BlockSpec(memory_space=pltpu.HBM)
MIB = 1024 * 1024


def call(body, outs, ins, flops, aliases=None, scratch=(), vmem=12, out_space=VM):
    return pl.pallas_call(
        body,
        out_shape=outs,
        in_specs=ins,
        out_specs=jax.tree.map(lambda _: out_space, outs),
        scratch_shapes=list(scratch),
        input_output_aliases=aliases or {},
        cost_estimate=pl.CostEstimate(flops=flops, bytes_accessed=MIB, transcendentals=0),
        compiler_params=pltpu.CompilerParams(vmem_limit_bytes=vmem * MIB),
    )


def sds(shape, dtype=F32):
    return jax.ShapeDtypeStruct(shape, dtype)


def core_index():
    return lax.axis_index("tok") & 1


def split3(x):
    hi = x.astype(BF16).astype(F32)
    rest = x - hi
    mid = rest.astype(BF16).astype(F32)
    return hi, mid, rest - mid


def prep_body(
    ld_hbm, v_hbm, k_hbm, d_ref, dcol_ref, vt_ref, own_ref, send_ref,
    state_ref, ld_ref, v_ref, k_ref, sems,
):
    pairs = ((ld_hbm, ld_ref), (v_hbm, v_ref), (k_hbm, k_ref))
    copies = [pltpu.make_async_copy(a, b, sems.at[i]) for i, (a, b) in enumerate(pairs)]
    for copy in copies:
        copy.start()
    core = core_index()
    copies[0].wait()
    ld = ld_ref[...]
    parts = jnp.concatenate([*split3(ld), jnp.zeros_like(ld)], axis=0).astype(BF16)
    row = lax.broadcasted_iota(jnp.int32, (BLOCK, BLOCK), 0)
    col = lax.broadcasted_iota(jnp.int32, (BLOCK, BLOCK), 1)
    upto = (row <= col).astype(F32).astype(BF16)
    sums = jnp.dot(parts, upto, preferred_element_type=F32)
    d = sums[0:8] + sums[8:16] + sums[16:24]
    d_ref[...] = d
    total = jnp.broadcast_to(d[:, BLOCK - 1 : BLOCK], (HEADS, BLOCK))
    toend = jnp.exp(total - d)
    copies[1].wait()
    vt = v_ref[...].T
    vt_ref[...] = vt
    scaled = [
        (vt[h * WIDTH : (h + 1) * WIDTH].astype(F32) * toend[h : h + 1]).astype(BF16)
        for h in range(HEADS)
    ]
    copies[2].wait()
    state_ref[...] = jnp.dot(
        jnp.concatenate(scaled, axis=0), k_ref[...], preferred_element_type=F32
    )
    own_ref[0:ROWS] = state_ref[pl.ds(pl.multiple_of(core * ROWS, ROWS), ROWS), :]
    own_ref[ROWS:BUF_ROWS] = total[:, 0:STATE]
    send_ref[0:ROWS] = state_ref[pl.ds(pl.multiple_of((1 - core) * ROWS, ROWS), ROWS), :]
    send_ref[ROWS:BUF_ROWS] = total[:, 0:STATE]
    dcol_ref[...] = d.T


def prep(ld, v, k):
    buf = sds((BUF_ROWS, STATE))
    outs = [sds((HEADS, BLOCK)), sds((BLOCK, HEADS)), sds((BLOCK, BLOCK), BF16)]
    outs += [buf, buf]
    return call(
        prep_body, outs, [HB] * 3, 10**7,
        scratch=[
            pltpu.VMEM((HEADS * WIDTH, STATE), F32),
            pltpu.VMEM((HEADS, BLOCK), F32),
            pltpu.VMEM((BLOCK, HEADS * WIDTH), BF16),
            pltpu.VMEM((BLOCK, STATE), BF16),
            pltpu.SemaphoreType.DMA((3,)),
        ],
    )(*(pltpu.with_memory_space_constraint(x, pltpu.HBM) for x in (ld, v, k)))


def merge_body(level, own_ref, got_ref, *refs):
    out_ref, fac_ref = refs[-2:]
    upper = ((lax.axis_index("tok") >> level) & 1) == 1
    own_ext = own_ref[ROWS:BUF_ROWS]
    got_ext = got_ref[ROWS:BUF_ROWS]
    one = jnp.ones_like(own_ext)
    fac_ref[0:HEADS] = jnp.where(upper, one, jnp.exp(got_ext))
    fac_ref[HEADS : 2 * HEADS] = jnp.where(upper, jnp.exp(own_ext), one)
    first = core_index() * HALF
    for j in range(HALF):
        rows = slice(j * WIDTH, (j + 1) * WIDTH)
        fa = fac_ref[pl.ds(first + j, 1), :]
        fb = fac_ref[pl.ds(first + (HEADS + j), 1), :]
        out_ref[rows] = own_ref[rows] * fa + got_ref[rows] * fb
    out_ref[ROWS:BUF_ROWS] = own_ext + got_ext


def merge(level, own, got, *tokens):
    return call(
        functools.partial(merge_body, level), sds((BUF_ROWS, STATE)),
        [VM] * (2 + len(tokens)), 10**5,
        scratch=[pltpu.VMEM((2 * HEADS, STATE), F32)], vmem=4,
    )(own, got, *tokens)


def aux_body(q_ref, gate_ref, qt_ref, gt_ref):
    qt = q_ref[...].T
    qt_ref[0:STATE] = qt
    qt_ref[STATE : 2 * STATE] = qt
    for j in range(4):
        cols = slice(j * 128, (j + 1) * 128)
        v = gate_ref[:, cols].T.astype(F32)
        gt_ref[cols] = v / (1.0 + jnp.exp(-v))


def aux(q, gate):
    return call(
        aux_body, [sds((2 * STATE, BLOCK), BF16), sds((BLOCK, BLOCK))], [VM] * 2, 10**7
    )(q, gate)


def near_body(first, k_ref, qt_ref, vt_ref, d_ref, dcol_ref, w_ref, skip_ref, token_ref, out_ref, sc_ref, mix_ref):
    sc_ref[...] = jnp.dot(k_ref[...], qt_ref[0:STATE], preferred_element_type=F32)
    half = BLOCK // 2
    mix_ref[half:BLOCK, 0:half] = jnp.zeros((half, half), BF16)
    mix_ref[128:256, 0:128] = jnp.zeros((128, 128), BF16)
    mix_ref[384:512, 256:384] = jnp.zeros((128, 128), BF16)
    srow = lax.broadcasted_iota(jnp.int32, (128, 128), 0)
    tcol = lax.broadcasted_iota(jnp.int32, (128, 128), 1)
    cross = srow ^ tcol
    causal = srow <= tcol
    for n in range(2):
        h = first + n
        for i in range(4):
            rows = slice(i * 128, (i + 1) * 128)
            dcol = jnp.broadcast_to(dcol_ref[rows, h : h + 1], (128, 128))
            for j in range(i, 4):
                cols = slice(j * 128, (j + 1) * 128)
                spread = d_ref[h : h + 1, cols] - dcol
                if i == j:
                    spread = jnp.where(causal, spread, -jnp.inf)
                    chosen = jnp.broadcast_to(w_ref[0, h : h + 1, cols], (128, 128))
                    for level in range(1, 8):
                        chosen = jnp.where(
                            cross >= 1 << (level - 1), w_ref[level, h : h + 1, cols], chosen
                        )
                else:
                    chosen = w_ref[7 + (i ^ j).bit_length(), h : h + 1, cols]
                mix_ref[rows, cols] = (sc_ref[rows, cols] * jnp.exp(spread) * chosen).astype(BF16)
        mine = slice(h * WIDTH, (h + 1) * WIDTH)
        here = slice(n * WIDTH, (n + 1) * WIDTH)
        vt = vt_ref[mine]
        skip = vt.astype(F32) * skip_ref[h]
        out_ref[here, 0:half] = skip[:, 0:half] + jnp.dot(
            vt[:, 0:half], mix_ref[0:half, 0:half], preferred_element_type=F32
        )
        out_ref[here, half:BLOCK] = skip[:, half:BLOCK] + jnp.dot(
            vt, mix_ref[:, half:BLOCK], preferred_element_type=F32
        )


def near(first, k, qt, vt, d, dcol, w, skip, token):
    return call(
        functools.partial(near_body, first), sds((2 * WIDTH, BLOCK)), [VM] * 6 + [SM, VM],
        10**7,
        scratch=[pltpu.VMEM((BLOCK, BLOCK), F32), pltpu.VMEM((BLOCK, BLOCK), BF16)],
    )(k, qt, vt, d, dcol, w, skip, token)


def readout(level, acc_rows, emit, qt_ref, d_ref, w_ref, lead_ref, buf_refs, coef_ref):
    upper = ((lax.axis_index("tok") >> level) & 1) == 1
    lead = lead_ref[...]
    gain = jnp.where(upper, jnp.exp(lead), 0.0)[:, 0:1]
    coef_ref[...] = w_ref[LOCAL_BITS + 1 + level] * jnp.exp(d_ref[...]) * gain
    core = core_index()
    for side, ref in zip((core, 1 - core), buf_refs):
        states = ref[0:ROWS]
        hi = states.astype(BF16)
        lo = (states - hi.astype(F32)).astype(BF16)
        read = jnp.dot(jnp.concatenate([hi, lo], axis=1), qt_ref[...], preferred_element_type=F32)
        for j in range(HALF):
            head = side * HALF + j
            row = pl.multiple_of(head * WIDTH, WIDTH)
            term = read[j * WIDTH : (j + 1) * WIDTH] * coef_ref[pl.ds(head, 1), :]
            emit(row, acc_rows(row) + term)
    got = buf_refs[0][ROWS:BUF_ROWS]
    return lead + jnp.where(upper, got, 0.0)


def far_body(level, qt_ref, d_ref, w_ref, lead_ref, *rest):
    coef_ref, next_ref, out_ref = rest[-1], rest[-2], rest[-3]
    bufs = rest[:2]

    def emit(row, value):
        out_ref[pl.ds(row, WIDTH), :] = value

    def start(row):
        return rest[2][pl.ds(row, WIDTH), :] if level > 0 else 0.0

    next_ref[...] = readout(level, start, emit, qt_ref, d_ref, w_ref, lead_ref, bufs, coef_ref)
    if level > 0:
        rows = slice((level - 1) * 2 * WIDTH, level * 2 * WIDTH)
        out_ref[rows] = out_ref[rows] + rest[3][...]


def far(level, qt, d, w, lead, bufs, *more):
    return call(
        functools.partial(far_body, level), [sds((BLOCK, BLOCK)), sds((HEADS, STATE))],
        [VM] * (6 + len(more)), 10**7,
        aliases={6: 0} if more else None,
        scratch=[pltpu.VMEM((HEADS, BLOCK), F32)],
    )(qt, d, w, lead, *bufs, *more)


def close_body(level, qt_ref, d_ref, w_ref, lead_ref, acc_ref, gt_ref, *rest):
    bufs, out_ref, sq_ref, coef_ref = rest[:2], rest[-3], rest[-2], rest[-1]
    sums = []

    def emit(row, value):
        gated = value * gt_ref[pl.ds(row, WIDTH), :]
        out_ref[pl.ds(row, WIDTH), :] = gated
        sums.append(jnp.sum(gated * gated, axis=0, keepdims=True))

    readout(
        level, lambda row: acc_ref[pl.ds(row, WIDTH), :], emit,
        qt_ref, d_ref, w_ref, lead_ref, bufs, coef_ref,
    )
    sq_ref[...] = sum(sums[1:], sums[0])


def close(level, qt, d, w, lead, acc, gt, bufs):
    return call(
        functools.partial(close_body, level), [sds((BLOCK, BLOCK)), sds((1, BLOCK))],
        [VM] * 8, 10**7,
        scratch=[pltpu.VMEM((HEADS, BLOCK), F32)],
    )(qt, d, w, lead, acc, gt, *bufs)


def turn_body(g_ref, gain_ref, out_ref):
    for j in range(4):
        rows = slice(j * 128, (j + 1) * 128)
        out_ref[rows] = g_ref[:, rows].T * gain_ref[...]


def turn(g, gain):
    return call(turn_body, sds((BLOCK, BLOCK)), [VM] * 2, 10**7)(g, gain)


def finish_body(width, g_ref, a_ref, b_ref, c_ref, e_ref, out_hbm, out_ref, sems):
    total = a_ref[...] + b_ref[...] + c_ref[...] + e_ref[...]
    scale = lax.rsqrt(total / width + epsilon)
    copies = []
    for j in range(4):
        rows = slice(j * 128, (j + 1) * 128)
        column = jnp.broadcast_to(scale[:, rows], (128, 128)).T
        for i in range(4):
            cols = slice(i * 128, (i + 1) * 128)
            out_ref[rows, cols] = (g_ref[rows, cols] * column).astype(BF16)
        copies.append(pltpu.make_async_copy(out_ref.at[rows], out_hbm.at[rows], sems.at[j]))
        copies[-1].start()
    for copy in copies:
        copy.wait()


def finish(width, g, sums):
    return call(
        functools.partial(finish_body, width), sds((BLOCK, BLOCK), BF16), [VM] * 5,
        10**8, out_space=HB,
        scratch=[pltpu.VMEM((BLOCK, BLOCK), BF16), pltpu.SemaphoreType.DMA((4,))],
    )(g, *sums)


def hop(x, axis, flip):
    count = lax.axis_size(axis)
    return lax.ppermute(x, axis, [(i, i ^ flip) for i in range(count)])


CORE, Z1, Z2, Z3, Z7, X1, X2, X3 = 1, 2, 4, 6, 14, 16, 32, 48


def work(head_inputs, state_keys, state_queries, log_decay, level_weight, skip_scale, gate_input, norm_gain):
    w = level_weight.transpose(2, 1, 0)
    d, dcol, vt, own, send = prep(log_decay.T, head_inputs, state_keys)
    swap = lambda x: hop(x, "tok", CORE)
    close_by = lambda first, token: near(
        first, state_keys, qt, vt, d, dcol, w, skip_scale, token
    )
    step = lambda level, lead, bufs, *more: far(level, qt, d, w, lead, bufs, *more)
    got = swap(send)
    qt, gt = aux(state_queries, gate_input)
    chip = merge(0, own, got, gt)
    levels = [(got, swap(own))]
    parts = [close_by(0, chip), close_by(2, chip)]
    z2 = hop(chip, "tok", Z2)
    z1 = hop(chip, "tok", Z1)
    z3 = hop(chip, "tok", Z3)
    pair = merge(1, chip, z1)
    across = merge(1, z2, z3)
    quad = merge(2, pair, across, *parts)
    levels += [(z1, swap(z1)), (across, swap(across))]
    parts.append(close_by(4, quad))
    acc, lead = step(0, jnp.zeros((HEADS, STATE), F32), levels[0])
    acc, lead = step(1, lead, levels[1], acc, parts[0])
    z7 = hop(quad, "tok", Z7)
    line = merge(3, quad, z7, parts[2], acc)
    levels.append((z7, swap(z7)))
    parts.append(close_by(6, line))
    acc, lead = step(2, lead, levels[2], acc, parts[1])
    x2 = hop(line, "tok", X2)
    x1 = hop(line, "tok", X1)
    x3 = hop(line, "tok", X3)
    levels.append((x1, swap(x1)))
    beyond = merge(4, x2, x3, parts[3], acc)
    levels.append((beyond, swap(beyond)))
    acc, lead = step(3, lead, levels[3], acc, parts[2])
    acc, lead = step(4, lead, levels[4], acc, parts[3])
    gated, squares = close(5, qt, d, w, lead, acc, gt, levels[5])
    shares = [hop(squares, "head", 2), hop(squares, "head", 1), hop(squares, "head", 3)]
    turned = turn(gated, norm_gain[None])
    return finish(HEADS * WIDTH * lax.axis_size("head"), turned, [squares, *shares])


def solution(mesh):
    return jax.shard_map(
        work,
        mesh=mesh,
        in_specs=(
            P("tok", "head"),
            P("tok", None),
            P("tok", None),
            P("tok", "head"),
            P("tok", "head", None),
            P("head"),
            P("tok", "head"),
            P("head"),
        ),
        out_specs=P("tok", "head"),
        check_vma=False,
    )
```

```python
import functools

import jax
import jax.numpy as jnp
from jax import lax
from jax.experimental import pallas as pl
from jax.experimental.pallas import tpu as pltpu
from jax.sharding import PartitionSpec as P


epsilon = 1e-05
BLOCK = 512
HEADS = 8
WIDTH = 64
STATE = 128
HALF = HEADS // 2
ROWS = HALF * WIDTH
BUF_ROWS = ROWS + HEADS
LOCAL_BITS = 9
F32 = jnp.float32
BF16 = jnp.bfloat16
VM = pl.BlockSpec(memory_space=pltpu.VMEM)
SM = pl.BlockSpec(memory_space=pltpu.SMEM)
HB = pl.BlockSpec(memory_space=pltpu.HBM)
MIB = 1024 * 1024


def call(body, outs, ins, flops, aliases=None, scratch=(), vmem=12, out_space=VM):
    return pl.pallas_call(
        body,
        out_shape=outs,
        in_specs=ins,
        out_specs=jax.tree.map(lambda _: out_space, outs),
        scratch_shapes=list(scratch),
        input_output_aliases=aliases or {},
        cost_estimate=pl.CostEstimate(flops=flops, bytes_accessed=MIB, transcendentals=0),
        compiler_params=pltpu.CompilerParams(vmem_limit_bytes=vmem * MIB),
    )


def sds(shape, dtype=F32):
    return jax.ShapeDtypeStruct(shape, dtype)


def core_index():
    return lax.axis_index("tok") & 1


def split3(x):
    hi = x.astype(BF16).astype(F32)
    rest = x - hi
    mid = rest.astype(BF16).astype(F32)
    return hi, mid, rest - mid


def prep_body(
    ld_hbm, v_hbm, k_hbm, d_ref, vt_ref, own_ref, send_ref, ld_ref, v_ref, k_ref, scaled_ref, sems
):
    pairs = ((v_hbm, v_ref), (ld_hbm, ld_ref), (k_hbm, k_ref))
    copies = [pltpu.make_async_copy(a, b, sems.at[i]) for i, (a, b) in enumerate(pairs)]
    for copy in copies:
        copy.start()
    core = core_index()
    row = lax.broadcasted_iota(jnp.int32, (128, 128), 0)
    col = lax.broadcasted_iota(jnp.int32, (128, 128), 1)
    upto = (row <= col).astype(F32).astype(BF16)
    copies[1].wait()
    terms = []
    for j in range(4):
        ld = ld_ref[:, j * 128 : (j + 1) * 128]
        terms += [*split3(ld), jnp.zeros_like(ld)]
    sums = jnp.dot(jnp.concatenate(terms, axis=0).astype(BF16), upto, preferred_element_type=F32)
    inner, totals = [], []
    for j in range(4):
        base = j * 32
        part = sums[base : base + 8] + sums[base + 8 : base + 16] + sums[base + 16 : base + 24]
        inner.append(part)
        totals.append(jnp.broadcast_to(part[:, 127:128], (HEADS, 128)))
    ahead = jnp.zeros((HEADS, 128), F32)
    d = []
    for j in range(4):
        d.append(inner[j] + ahead)
        ahead = ahead + totals[j]
    total = ahead
    toend = jnp.concatenate([jnp.exp(total - x) for x in d], axis=1)
    for j in range(4):
        d_ref[:, j * 128 : (j + 1) * 128] = d[j]
    copies[0].wait()
    vt = v_ref[...].T
    for h in range(HEADS):
        rows = slice(h * WIDTH, (h + 1) * WIDTH)
        scaled_ref[rows] = (vt[rows].astype(F32) * toend[h : h + 1]).astype(BF16)
    copies[2].wait()
    keys = k_ref[...]
    for ref, side in ((send_ref, 1 - core), (own_ref, core)):
        rows = pl.ds(pl.multiple_of(side * ROWS, ROWS), ROWS)
        ref[0:ROWS] = jnp.dot(scaled_ref[rows, :], keys, preferred_element_type=F32)
        ref[ROWS:BUF_ROWS] = total
    vt_ref[...] = vt


def prep(ld, v, k):
    buf = sds((BUF_ROWS, STATE))
    outs = [sds((HEADS, BLOCK)), sds((BLOCK, BLOCK), BF16), buf, buf]
    return call(
        prep_body, outs, [HB] * 3, 10**7,
        scratch=[
            pltpu.VMEM((HEADS, BLOCK), F32),
            pltpu.VMEM((BLOCK, HEADS * WIDTH), BF16),
            pltpu.VMEM((BLOCK, STATE), BF16),
            pltpu.VMEM((HEADS * WIDTH, BLOCK), BF16),
            pltpu.SemaphoreType.DMA((3,)),
        ],
    )(*(pltpu.with_memory_space_constraint(x, pltpu.HBM) for x in (ld, v, k)))


def merge_body(level, own_ref, got_ref, *refs):
    out_ref, fac_ref = refs[-2:]
    upper = ((lax.axis_index("tok") >> level) & 1) == 1
    own_ext = own_ref[ROWS:BUF_ROWS]
    got_ext = got_ref[ROWS:BUF_ROWS]
    one = jnp.ones_like(own_ext)
    fac_ref[0:HEADS] = jnp.where(upper, one, jnp.exp(got_ext))
    fac_ref[HEADS : 2 * HEADS] = jnp.where(upper, jnp.exp(own_ext), one)
    first = core_index() * HALF
    for j in range(HALF):
        rows = slice(j * WIDTH, (j + 1) * WIDTH)
        fa = fac_ref[pl.ds(first + j, 1), :]
        fb = fac_ref[pl.ds(first + (HEADS + j), 1), :]
        out_ref[rows] = own_ref[rows] * fa + got_ref[rows] * fb
    out_ref[ROWS:BUF_ROWS] = own_ext + got_ext


def merge(level, own, got, *tokens):
    return call(
        functools.partial(merge_body, level), sds((BUF_ROWS, STATE)),
        [VM] * (2 + len(tokens)), 10**5,
        scratch=[pltpu.VMEM((2 * HEADS, STATE), F32)], vmem=4,
    )(own, got, *tokens)


def aux_body(q_ref, gate_ref, d_ref, qt_ref, gt_ref, dcol_ref):
    qt = q_ref[...].T
    qt_ref[0:STATE] = qt
    qt_ref[STATE : 2 * STATE] = qt
    for j in range(4):
        cols = slice(j * 128, (j + 1) * 128)
        v = gate_ref[:, cols].T.astype(F32)
        gt_ref[cols] = v / (1.0 + jnp.exp(-v))
    dcol_ref[...] = d_ref[...].T


def aux(q, gate, d):
    outs = [sds((2 * STATE, BLOCK), BF16), sds((BLOCK, BLOCK)), sds((BLOCK, HEADS))]
    return call(aux_body, outs, [VM] * 3, 10**7)(q, gate, d)


def near_body(first, k_ref, qt_ref, vt_ref, d_ref, dcol_ref, w_ref, skip_ref, token_ref, out_ref, sc_ref, mix_ref):
    sc_ref[...] = jnp.dot(k_ref[...], qt_ref[0:STATE], preferred_element_type=F32)
    half = BLOCK // 2
    mix_ref[half:BLOCK, 0:half] = jnp.zeros((half, half), BF16)
    mix_ref[128:256, 0:128] = jnp.zeros((128, 128), BF16)
    mix_ref[384:512, 256:384] = jnp.zeros((128, 128), BF16)
    srow = lax.broadcasted_iota(jnp.int32, (128, 128), 0)
    tcol = lax.broadcasted_iota(jnp.int32, (128, 128), 1)
    cross = srow ^ tcol
    causal = srow <= tcol
    for n in range(2):
        h = first + n
        for i in range(4):
            rows = slice(i * 128, (i + 1) * 128)
            dcol = jnp.broadcast_to(dcol_ref[rows, h : h + 1], (128, 128))
            for j in range(i, 4):
                cols = slice(j * 128, (j + 1) * 128)
                spread = d_ref[h : h + 1, cols] - dcol
                if i == j:
                    spread = jnp.where(causal, spread, -jnp.inf)
                    chosen = jnp.broadcast_to(w_ref[0, h : h + 1, cols], (128, 128))
                    for level in range(1, 8):
                        chosen = jnp.where(
                            cross >= 1 << (level - 1), w_ref[level, h : h + 1, cols], chosen
                        )
                else:
                    chosen = w_ref[7 + (i ^ j).bit_length(), h : h + 1, cols]
                mix_ref[rows, cols] = (sc_ref[rows, cols] * jnp.exp(spread) * chosen).astype(BF16)
        mine = slice(h * WIDTH, (h + 1) * WIDTH)
        here = slice(n * WIDTH, (n + 1) * WIDTH)
        vt = vt_ref[mine]
        skip = vt.astype(F32) * skip_ref[h]
        out_ref[here, 0:half] = skip[:, 0:half] + jnp.dot(
            vt[:, 0:half], mix_ref[0:half, 0:half], preferred_element_type=F32
        )
        out_ref[here, half:BLOCK] = skip[:, half:BLOCK] + jnp.dot(
            vt, mix_ref[:, half:BLOCK], preferred_element_type=F32
        )


def near(first, k, qt, vt, d, dcol, w, skip, token):
    return call(
        functools.partial(near_body, first), sds((2 * WIDTH, BLOCK)), [VM] * 6 + [SM, VM],
        10**7,
        scratch=[pltpu.VMEM((BLOCK, BLOCK), F32), pltpu.VMEM((BLOCK, BLOCK), BF16)],
    )(k, qt, vt, d, dcol, w, skip, token)


def readout(level, sides, acc_rows, emit, qt_ref, d_ref, w_ref, lead, buf_refs, coef_ref):
    upper = ((lax.axis_index("tok") >> level) & 1) == 1
    gain = jnp.where(upper, jnp.exp(lead), 0.0)[:, 0:1]
    coef_ref[...] = w_ref[LOCAL_BITS + 1 + level] * jnp.exp(d_ref[...]) * gain
    core = core_index()
    for n, ref in zip(sides, buf_refs):
        side = core if n == 0 else 1 - core
        states = ref[0:ROWS]
        hi = states.astype(BF16)
        lo = (states - hi.astype(F32)).astype(BF16)
        read = jnp.dot(jnp.concatenate([hi, lo], axis=1), qt_ref[...], preferred_element_type=F32)
        for j in range(HALF):
            head = side * HALF + j
            row = pl.multiple_of(head * WIDTH, WIDTH)
            term = read[j * WIDTH : (j + 1) * WIDTH] * coef_ref[pl.ds(head, 1), :]
            emit(row, acc_rows(row) + term)


def far_body(level, qt_ref, d_ref, w_ref, lead_ref, *rest):
    coef_ref, next_ref, out_ref = rest[-1], rest[-2], rest[-3]
    bufs = rest[:2]

    def emit(row, value):
        out_ref[pl.ds(row, WIDTH), :] = value

    def start(row):
        return rest[2][pl.ds(row, WIDTH), :] if level > 0 else 0.0

    lead = lead_ref[...]
    readout(level, (0, 1), start, emit, qt_ref, d_ref, w_ref, lead, bufs, coef_ref)
    upper = ((lax.axis_index("tok") >> level) & 1) == 1
    next_ref[...] = lead + jnp.where(upper, bufs[0][ROWS:BUF_ROWS], 0.0)
    if level > 0:
        rows = slice((level - 1) * 2 * WIDTH, level * 2 * WIDTH)
        out_ref[rows] = out_ref[rows] + rest[3][...]


def far(level, qt, d, w, lead, bufs, *more):
    return call(
        functools.partial(far_body, level), [sds((BLOCK, BLOCK)), sds((HEADS, STATE))],
        [VM] * (6 + len(more)), 10**7,
        aliases={6: 0} if more else None,
        scratch=[pltpu.VMEM((HEADS, BLOCK), F32)],
    )(qt, d, w, lead, *bufs, *more)


def close_body(level, side, qt_ref, d_ref, w_ref, lead_ref, acc_ref, gt_ref, buf_ref, *rest):
    out_ref, sq_ref, coef_ref = rest[-3:]
    sums = [] if side == 0 else [rest[0][...]]
    half = core_index() if side == 0 else 1 - core_index()

    def emit(row, value):
        gated = value * gt_ref[pl.ds(row, WIDTH), :]
        out_ref[pl.ds(pl.multiple_of(row - half * ROWS, WIDTH), WIDTH), :] = gated
        sums.append(jnp.sum(gated * gated, axis=0, keepdims=True))

    readout(
        level, (side,), lambda row: acc_ref[pl.ds(row, WIDTH), :], emit,
        qt_ref, d_ref, w_ref, lead_ref[...], (buf_ref,), coef_ref,
    )
    sq_ref[...] = sum(sums[1:], sums[0])


def close(level, side, qt, d, w, lead, acc, gt, buf, *more):
    return call(
        functools.partial(close_body, level, side), [sds((ROWS, BLOCK)), sds((1, BLOCK))],
        [VM] * (7 + len(more)), 10**7,
        scratch=[pltpu.VMEM((HEADS, BLOCK), F32)],
    )(qt, d, w, lead, acc, gt, buf, *more)


def turn_body(own_ref, other_ref, gain_ref, out_ref):
    core = core_index()
    for ref, side in ((own_ref, core), (other_ref, 1 - core)):
        cols = pl.ds(pl.multiple_of(side * ROWS, ROWS), ROWS)
        gain = gain_ref[:, cols]
        for j in range(4):
            rows = slice(j * 128, (j + 1) * 128)
            out_ref[rows, cols] = ref[:, rows].T * gain


def turn(own, other, gain):
    return call(turn_body, sds((BLOCK, BLOCK)), [VM] * 3, 10**7)(own, other, gain)


def finish_body(width, g_ref, a_ref, b_ref, c_ref, e_ref, out_hbm, out_ref, sems):
    total = a_ref[...] + b_ref[...] + c_ref[...] + e_ref[...]
    scale = lax.rsqrt(total / width + epsilon)
    copies = []
    for j in range(4):
        rows = slice(j * 128, (j + 1) * 128)
        column = jnp.broadcast_to(scale[:, rows], (128, 128)).T
        for i in range(4):
            cols = slice(i * 128, (i + 1) * 128)
            out_ref[rows, cols] = (g_ref[rows, cols] * column).astype(BF16)
        copies.append(pltpu.make_async_copy(out_ref.at[rows], out_hbm.at[rows], sems.at[j]))
        copies[-1].start()
    for copy in copies:
        copy.wait()


def finish(width, g, sums):
    return call(
        functools.partial(finish_body, width), sds((BLOCK, BLOCK), BF16), [VM] * 5,
        10**8, out_space=HB,
        scratch=[pltpu.VMEM((BLOCK, BLOCK), BF16), pltpu.SemaphoreType.DMA((4,))],
    )(g, *sums)


def hop(x, axis, flip):
    count = lax.axis_size(axis)
    return lax.ppermute(x, axis, [(i, i ^ flip) for i in range(count)])


CORE, Z1, Z3, Z7, X1, X2, X3 = 1, 2, 6, 14, 16, 32, 48


def work(head_inputs, state_keys, state_queries, log_decay, level_weight, skip_scale, gate_input, norm_gain):
    w = level_weight.transpose(2, 1, 0)
    d, vt, own, send = prep(log_decay.T, head_inputs, state_keys)
    swap = lambda x: hop(x, "tok", CORE)

    def close_by(first, token):
        return near(first, state_keys, qt, vt, d, dcol, w, skip_scale, token)

    def step(level, lead, bufs, *more):
        return far(level, qt, d, w, lead, bufs, *more)

    got = swap(send)
    qt, gt, dcol = aux(state_queries, gate_input, d)
    chip = merge(0, own, got, gt)
    levels = [(got, swap(own))]
    parts = [close_by(0, chip)]
    z1 = hop(chip, "tok", Z1)
    pair = merge(1, chip, z1, parts[0])
    levels.append((z1, swap(z1)))
    parts.append(close_by(2, pair))
    acc, lead = step(0, jnp.zeros((HEADS, STATE), F32), levels[0])
    z3 = hop(pair, "tok", Z3)
    quad = merge(2, pair, z3, parts[1], acc)
    levels.append((z3, swap(z3)))
    parts.append(close_by(4, quad))
    acc, lead = step(1, lead, levels[1], acc, parts[0])
    z7 = hop(quad, "tok", Z7)
    acc, lead = step(2, lead, levels[2], acc, parts[1])
    line = merge(3, quad, z7, parts[2], acc)
    levels.append((z7, swap(z7)))
    parts.append(close_by(6, line))
    acc, lead = step(3, lead, levels[3], acc, parts[2])
    x2 = hop(line, "tok", X2)
    x1 = hop(line, "tok", X1)
    x3 = hop(line, "tok", X3)
    levels.append((x1, swap(x1)))
    beyond = merge(4, x2, x3, parts[3], acc)
    other = swap(beyond)
    acc, lead = step(4, lead, levels[4], acc, parts[3])
    last = (qt, d, w, lead, acc, gt)
    mine, part = close(5, 0, *last, beyond)
    rest, squares = close(5, 1, *last, other, part)
    shares = [hop(squares, "head", 2), hop(squares, "head", 1), hop(squares, "head", 3)]
    turned = turn(mine, rest, norm_gain[None])
    return finish(HEADS * WIDTH * lax.axis_size("head"), turned, [squares, *shares])


def solution(mesh):
    return jax.shard_map(
        work,
        mesh=mesh,
        in_specs=(
            P("tok", "head"),
            P("tok", None),
            P("tok", None),
            P("tok", "head"),
            P("tok", "head", None),
            P("head"),
            P("tok", "head"),
            P("head"),
        ),
        out_specs=P("tok", "head"),
        check_vma=False,
    )
```

```python
import functools

import jax
import jax.numpy as jnp
from jax import lax
from jax.experimental import pallas as pl
from jax.experimental.pallas import tpu as pltpu
from jax.sharding import PartitionSpec as P


epsilon = 1e-05
BLOCK = 512
HEADS = 8
WIDTH = 64
STATE = 128
HALF = HEADS // 2
ROWS = HALF * WIDTH
BUF_ROWS = ROWS + HEADS
LOCAL_BITS = 9
F32 = jnp.float32
BF16 = jnp.bfloat16
VM = pl.BlockSpec(memory_space=pltpu.VMEM)
SM = pl.BlockSpec(memory_space=pltpu.SMEM)
HB = pl.BlockSpec(memory_space=pltpu.HBM)
MIB = 1024 * 1024


def call(body, outs, ins, flops, aliases=None, scratch=(), vmem=12, out_space=VM):
    return pl.pallas_call(
        body,
        out_shape=outs,
        in_specs=ins,
        out_specs=jax.tree.map(lambda _: out_space, outs),
        scratch_shapes=list(scratch),
        input_output_aliases=aliases or {},
        cost_estimate=pl.CostEstimate(flops=flops, bytes_accessed=MIB, transcendentals=0),
        compiler_params=pltpu.CompilerParams(vmem_limit_bytes=vmem * MIB),
    )


def sds(shape, dtype=F32):
    return jax.ShapeDtypeStruct(shape, dtype)


def core_index():
    return lax.axis_index("tok") & 1


def split3(x):
    hi = x.astype(BF16).astype(F32)
    rest = x - hi
    mid = rest.astype(BF16).astype(F32)
    return hi, mid, rest - mid


def product(v, toend_ref, total, side, keys, out_ref):
    vt = v.T
    scaled = [
        (vt[j * WIDTH : (j + 1) * WIDTH].astype(F32) * toend_ref[pl.ds(side * HALF + j, 1), :])
        .astype(BF16)
        for j in range(HALF)
    ]
    out_ref[0:ROWS] = jnp.dot(
        jnp.concatenate(scaled, axis=0), keys, preferred_element_type=F32
    )
    out_ref[ROWS:BUF_ROWS] = total


def prep_body(
    ld_hbm, v_hbm, k_hbm, d_ref, toend_ref, total_ref, send_ref, mine_ref, k_ref,
    ld_ref, theirs_ref, sems,
):
    me = core_index()
    columns = lambda side: pl.ds(pl.multiple_of(side * ROWS, ROWS), ROWS)
    pairs = (
        (v_hbm.at[:, columns(1 - me)], theirs_ref), (ld_hbm, ld_ref), (k_hbm, k_ref),
        (v_hbm.at[:, columns(me)], mine_ref),
    )
    copies = [pltpu.make_async_copy(a, b, sems.at[i]) for i, (a, b) in enumerate(pairs)]
    for copy in copies:
        copy.start()
    row = lax.broadcasted_iota(jnp.int32, (128, 128), 0)
    col = lax.broadcasted_iota(jnp.int32, (128, 128), 1)
    upto = (row <= col).astype(F32).astype(BF16)
    copies[1].wait()
    terms = []
    for j in range(4):
        ld = ld_ref[:, j * 128 : (j + 1) * 128]
        terms += [*split3(ld), jnp.zeros_like(ld)]
    sums = jnp.dot(jnp.concatenate(terms, axis=0).astype(BF16), upto, preferred_element_type=F32)
    inner, totals = [], []
    for j in range(4):
        base = j * 32
        part = sums[base : base + 8] + sums[base + 8 : base + 16] + sums[base + 16 : base + 24]
        inner.append(part)
        totals.append(jnp.broadcast_to(part[:, 127:128], (HEADS, 128)))
    ahead = jnp.zeros((HEADS, 128), F32)
    d = []
    for j in range(4):
        d.append(inner[j] + ahead)
        ahead = ahead + totals[j]
    total = ahead
    total_ref[...] = total
    for j in range(4):
        cols = slice(j * 128, (j + 1) * 128)
        d_ref[:, cols] = d[j]
        toend_ref[:, cols] = jnp.exp(total - d[j])
    copies[0].wait()
    copies[2].wait()
    product(theirs_ref[...], toend_ref, total, 1 - me, k_ref[...], send_ref)
    copies[3].wait()


def prep(ld, v, k):
    outs = [sds((HEADS, BLOCK)), sds((HEADS, BLOCK)), sds((HEADS, 128)), sds((BUF_ROWS, STATE))]
    outs += [sds((BLOCK, ROWS), BF16), sds((BLOCK, STATE), BF16)]
    return call(
        prep_body, outs, [HB] * 3, 10**7,
        scratch=[
            pltpu.VMEM((HEADS, BLOCK), F32),
            pltpu.VMEM((BLOCK, ROWS), BF16),
            pltpu.SemaphoreType.DMA((4,)),
        ],
    )(*(pltpu.with_memory_space_constraint(x, pltpu.HBM) for x in (ld, v, k)))


def own_body(v_ref, k_ref, toend_ref, total_ref, out_ref):
    product(v_ref[...], toend_ref, total_ref[...], core_index(), k_ref[...], out_ref)


def own_state(v, k, toend, total):
    return call(own_body, sds((BUF_ROWS, STATE)), [VM] * 4, 10**6)(v, k, toend, total)


def merge_body(level, own_ref, got_ref, *refs):
    out_ref, fac_ref = refs[-2:]
    upper = ((lax.axis_index("tok") >> level) & 1) == 1
    own_ext = own_ref[ROWS:BUF_ROWS]
    got_ext = got_ref[ROWS:BUF_ROWS]
    one = jnp.ones_like(own_ext)
    fac_ref[0:HEADS] = jnp.where(upper, one, jnp.exp(got_ext))
    fac_ref[HEADS : 2 * HEADS] = jnp.where(upper, jnp.exp(own_ext), one)
    first = core_index() * HALF
    for j in range(HALF):
        rows = slice(j * WIDTH, (j + 1) * WIDTH)
        fa = fac_ref[pl.ds(first + j, 1), :]
        fb = fac_ref[pl.ds(first + (HEADS + j), 1), :]
        out_ref[rows] = own_ref[rows] * fa + got_ref[rows] * fb
    out_ref[ROWS:BUF_ROWS] = own_ext + got_ext


def merge(level, own, got, *tokens):
    return call(
        functools.partial(merge_body, level), sds((BUF_ROWS, STATE)),
        [VM] * (2 + len(tokens)), 10**5,
        scratch=[pltpu.VMEM((2 * HEADS, STATE), F32)], vmem=4,
    )(own, got, *tokens)


def aux_body(q_ref, gate_ref, d_ref, v_ref, qt_ref, gt_ref, dcol_ref, vt_ref):
    qt = q_ref[...].T
    qt_ref[0:STATE] = qt
    qt_ref[STATE : 2 * STATE] = qt
    vt_ref[...] = v_ref[...].T
    dcol_ref[...] = d_ref[...].T
    for j in range(4):
        cols = slice(j * 128, (j + 1) * 128)
        v = gate_ref[:, cols].T.astype(F32)
        gt_ref[cols] = v / (1.0 + jnp.exp(-v))


def aux(q, gate, d, v):
    outs = [sds((2 * STATE, BLOCK), BF16), sds((BLOCK, BLOCK)), sds((BLOCK, HEADS))]
    outs += [sds((BLOCK, BLOCK), BF16)]
    return call(aux_body, outs, [VM] * 4, 10**7)(q, gate, d, v)


def near_body(first, k_ref, qt_ref, vt_ref, d_ref, dcol_ref, w_ref, skip_ref, token_ref, out_ref, sc_ref, mix_ref):
    sc_ref[...] = jnp.dot(k_ref[...], qt_ref[0:STATE], preferred_element_type=F32)
    half = BLOCK // 2
    mix_ref[half:BLOCK, 0:half] = jnp.zeros((half, half), BF16)
    mix_ref[128:256, 0:128] = jnp.zeros((128, 128), BF16)
    mix_ref[384:512, 256:384] = jnp.zeros((128, 128), BF16)
    srow = lax.broadcasted_iota(jnp.int32, (128, 128), 0)
    tcol = lax.broadcasted_iota(jnp.int32, (128, 128), 1)
    cross = srow ^ tcol
    causal = srow <= tcol
    for n in range(2):
        h = first + n
        for i in range(4):
            rows = slice(i * 128, (i + 1) * 128)
            dcol = jnp.broadcast_to(dcol_ref[rows, h : h + 1], (128, 128))
            for j in range(i, 4):
                cols = slice(j * 128, (j + 1) * 128)
                spread = d_ref[h : h + 1, cols] - dcol
                if i == j:
                    spread = jnp.where(causal, spread, -jnp.inf)
                    chosen = jnp.broadcast_to(w_ref[0, h : h + 1, cols], (128, 128))
                    for level in range(1, 8):
                        chosen = jnp.where(
                            cross >= 1 << (level - 1), w_ref[level, h : h + 1, cols], chosen
                        )
                else:
                    chosen = w_ref[7 + (i ^ j).bit_length(), h : h + 1, cols]
                mix_ref[rows, cols] = (sc_ref[rows, cols] * jnp.exp(spread) * chosen).astype(BF16)
        mine = slice(h * WIDTH, (h + 1) * WIDTH)
        here = slice(n * WIDTH, (n + 1) * WIDTH)
        vt = vt_ref[mine]
        skip = vt.astype(F32) * skip_ref[h]
        out_ref[here, 0:half] = skip[:, 0:half] + jnp.dot(
            vt[:, 0:half], mix_ref[0:half, 0:half], preferred_element_type=F32
        )
        out_ref[here, half:BLOCK] = skip[:, half:BLOCK] + jnp.dot(
            vt, mix_ref[:, half:BLOCK], preferred_element_type=F32
        )


def near(first, k, qt, vt, d, dcol, w, skip, token):
    return call(
        functools.partial(near_body, first), sds((2 * WIDTH, BLOCK)), [VM] * 6 + [SM, VM],
        10**7,
        scratch=[pltpu.VMEM((BLOCK, BLOCK), F32), pltpu.VMEM((BLOCK, BLOCK), BF16)],
    )(k, qt, vt, d, dcol, w, skip, token)


def readout(level, sides, acc_rows, emit, qt_ref, d_ref, w_ref, lead, buf_refs, coef_ref):
    upper = ((lax.axis_index("tok") >> level) & 1) == 1
    gain = jnp.where(upper, jnp.exp(lead), 0.0)[:, 0:1]
    coef_ref[...] = w_ref[LOCAL_BITS + 1 + level] * jnp.exp(d_ref[...]) * gain
    core = core_index()
    for n, ref in zip(sides, buf_refs):
        side = core if n == 0 else 1 - core
        states = ref[0:ROWS]
        hi = states.astype(BF16)
        lo = (states - hi.astype(F32)).astype(BF16)
        read = jnp.dot(jnp.concatenate([hi, lo], axis=1), qt_ref[...], preferred_element_type=F32)
        for j in range(HALF):
            head = side * HALF + j
            row = pl.multiple_of(head * WIDTH, WIDTH)
            term = read[j * WIDTH : (j + 1) * WIDTH] * coef_ref[pl.ds(head, 1), :]
            emit(row, acc_rows(row) + term)


def far_body(level, qt_ref, d_ref, w_ref, lead_ref, *rest):
    coef_ref, next_ref, out_ref = rest[-1], rest[-2], rest[-3]
    bufs = rest[:2]

    def emit(row, value):
        out_ref[pl.ds(row, WIDTH), :] = value

    def start(row):
        return rest[2][pl.ds(row, WIDTH), :] if level > 0 else 0.0

    lead = lead_ref[...]
    readout(level, (0, 1), start, emit, qt_ref, d_ref, w_ref, lead, bufs, coef_ref)
    upper = ((lax.axis_index("tok") >> level) & 1) == 1
    next_ref[...] = lead + jnp.where(upper, bufs[0][ROWS:BUF_ROWS], 0.0)
    if level > 0:
        rows = slice((level - 1) * 2 * WIDTH, level * 2 * WIDTH)
        out_ref[rows] = out_ref[rows] + rest[3][...]


def far(level, qt, d, w, lead, bufs, *more):
    return call(
        functools.partial(far_body, level), [sds((BLOCK, BLOCK)), sds((HEADS, STATE))],
        [VM] * (6 + len(more)), 10**7,
        aliases={6: 0} if more else None,
        scratch=[pltpu.VMEM((HEADS, BLOCK), F32)],
    )(qt, d, w, lead, *bufs, *more)


def close_body(level, side, qt_ref, d_ref, w_ref, lead_ref, acc_ref, gt_ref, buf_ref, *rest):
    out_ref, sq_ref, coef_ref = rest[-3:]
    sums = [] if side == 0 else [rest[0][...]]
    half = core_index() if side == 0 else 1 - core_index()

    def emit(row, value):
        gated = value * gt_ref[pl.ds(row, WIDTH), :]
        out_ref[pl.ds(pl.multiple_of(row - half * ROWS, WIDTH), WIDTH), :] = gated
        sums.append(jnp.sum(gated * gated, axis=0, keepdims=True))

    readout(
        level, (side,), lambda row: acc_ref[pl.ds(row, WIDTH), :], emit,
        qt_ref, d_ref, w_ref, lead_ref[...], (buf_ref,), coef_ref,
    )
    sq_ref[...] = sum(sums[1:], sums[0])


def close(level, side, qt, d, w, lead, acc, gt, buf, *more):
    return call(
        functools.partial(close_body, level, side), [sds((ROWS, BLOCK)), sds((1, BLOCK))],
        [VM] * (7 + len(more)), 10**7,
        scratch=[pltpu.VMEM((HEADS, BLOCK), F32)],
    )(qt, d, w, lead, acc, gt, buf, *more)


def turn_body(own_ref, other_ref, gain_ref, out_ref):
    core = core_index()
    for ref, side in ((own_ref, core), (other_ref, 1 - core)):
        cols = pl.ds(pl.multiple_of(side * ROWS, ROWS), ROWS)
        gain = gain_ref[:, cols]
        for j in range(4):
            rows = slice(j * 128, (j + 1) * 128)
            out_ref[rows, cols] = ref[:, rows].T * gain


def turn(own, other, gain):
    return call(turn_body, sds((BLOCK, BLOCK)), [VM] * 3, 10**7)(own, other, gain)


def finish_body(width, g_ref, a_ref, b_ref, c_ref, e_ref, out_hbm, out_ref, sems):
    total = a_ref[...] + b_ref[...] + c_ref[...] + e_ref[...]
    scale = lax.rsqrt(total / width + epsilon)
    copies = []
    for j in range(4):
        rows = slice(j * 128, (j + 1) * 128)
        column = jnp.broadcast_to(scale[:, rows], (128, 128)).T
        for i in range(4):
            cols = slice(i * 128, (i + 1) * 128)
            out_ref[rows, cols] = (g_ref[rows, cols] * column).astype(BF16)
        copies.append(pltpu.make_async_copy(out_ref.at[rows], out_hbm.at[rows], sems.at[j]))
        copies[-1].start()
    for copy in copies:
        copy.wait()


def finish(width, g, sums):
    return call(
        functools.partial(finish_body, width), sds((BLOCK, BLOCK), BF16), [VM] * 5,
        10**8, out_space=HB,
        scratch=[pltpu.VMEM((BLOCK, BLOCK), BF16), pltpu.SemaphoreType.DMA((4,))],
    )(g, *sums)


def hop(x, axis, flip):
    count = lax.axis_size(axis)
    return lax.ppermute(x, axis, [(i, i ^ flip) for i in range(count)])


CORE, Z1, Z3, Z7, X1, X2, X3 = 1, 2, 6, 14, 16, 32, 48


def work(head_inputs, state_keys, state_queries, log_decay, level_weight, skip_scale, gate_input, norm_gain):
    w = level_weight.transpose(2, 1, 0)
    d, toend, total, send, mine, keys = prep(log_decay.T, head_inputs, state_keys)
    swap = lambda x: hop(x, "tok", CORE)

    def close_by(first, token):
        return near(first, keys, qt, vt, d, dcol, w, skip_scale, token)

    def step(level, lead, bufs, *more):
        return far(level, qt, d, w, lead, bufs, *more)

    got = swap(send)
    own = own_state(mine, keys, toend, total)
    chip = merge(0, own, got)
    qt, gt, dcol, vt = aux(state_queries, gate_input, d, head_inputs)
    levels = [(got, swap(own))]
    parts = [close_by(0, chip)]
    z1 = hop(chip, "tok", Z1)
    pair = merge(1, chip, z1, parts[0])
    levels.append((z1, swap(z1)))
    parts.append(close_by(2, pair))
    acc, lead = step(0, jnp.zeros((HEADS, STATE), F32), levels[0])
    z3 = hop(pair, "tok", Z3)
    quad = merge(2, pair, z3, parts[1], acc)
    levels.append((z3, swap(z3)))
    parts.append(close_by(4, quad))
    acc, lead = step(1, lead, levels[1], acc, parts[0])
    z7 = hop(quad, "tok", Z7)
    acc, lead = step(2, lead, levels[2], acc, parts[1])
    line = merge(3, quad, z7, parts[2], acc)
    levels.append((z7, swap(z7)))
    parts.append(close_by(6, line))
    acc, lead = step(3, lead, levels[3], acc, parts[2])
    x2 = hop(line, "tok", X2)
    x1 = hop(line, "tok", X1)
    x3 = hop(line, "tok", X3)
    levels.append((x1, swap(x1)))
    beyond = merge(4, x2, x3, parts[3], acc)
    other = swap(beyond)
    acc, lead = step(4, lead, levels[4], acc, parts[3])
    last = (qt, d, w, lead, acc, gt)
    near_half, part = close(5, 0, *last, beyond)
    rest, squares = close(5, 1, *last, other, part)
    shares = [hop(squares, "head", 2), hop(squares, "head", 1), hop(squares, "head", 3)]
    turned = turn(near_half, rest, norm_gain[None])
    return finish(HEADS * WIDTH * lax.axis_size("head"), turned, [squares, *shares])


def solution(mesh):
    return jax.shard_map(
        work,
        mesh=mesh,
        in_specs=(
            P("tok", "head"),
            P("tok", None),
            P("tok", None),
            P("tok", "head"),
            P("tok", "head", None),
            P("head"),
            P("tok", "head"),
            P("head"),
        ),
        out_specs=P("tok", "head"),
        check_vma=False,
    )
```

```python
import functools

import jax
import jax.numpy as jnp
from jax import lax
from jax.experimental import pallas as pl
from jax.experimental.pallas import tpu as pltpu
from jax.sharding import PartitionSpec as P


epsilon = 1e-05
BLOCK = 512
HEADS = 8
WIDTH = 64
STATE = 128
HALF = HEADS // 2
ROWS = HALF * WIDTH
BUF_ROWS = ROWS + HEADS
LOCAL_BITS = 9
F32 = jnp.float32
BF16 = jnp.bfloat16
VM = pl.BlockSpec(memory_space=pltpu.VMEM)
SM = pl.BlockSpec(memory_space=pltpu.SMEM)
HB = pl.BlockSpec(memory_space=pltpu.HBM)
MIB = 1024 * 1024


def call(body, outs, ins, flops, aliases=None, scratch=(), vmem=12, out_space=VM):
    return pl.pallas_call(
        body,
        out_shape=outs,
        in_specs=ins,
        out_specs=jax.tree.map(lambda _: out_space, outs),
        scratch_shapes=list(scratch),
        input_output_aliases=aliases or {},
        cost_estimate=pl.CostEstimate(flops=flops, bytes_accessed=MIB, transcendentals=0),
        compiler_params=pltpu.CompilerParams(vmem_limit_bytes=vmem * MIB),
    )


def sds(shape, dtype=F32):
    return jax.ShapeDtypeStruct(shape, dtype)


def core_index():
    return lax.axis_index("tok") & 1


def split3(x):
    hi = x.astype(BF16).astype(F32)
    rest = x - hi
    mid = rest.astype(BF16).astype(F32)
    return hi, mid, rest - mid


def product(v, toend_ref, total, side, keys, out_ref):
    vt = v.T
    scaled = [
        (vt[j * WIDTH : (j + 1) * WIDTH].astype(F32) * toend_ref[pl.ds(side * HALF + j, 1), :])
        .astype(BF16)
        for j in range(HALF)
    ]
    out_ref[0:ROWS] = jnp.dot(
        jnp.concatenate(scaled, axis=0), keys, preferred_element_type=F32
    )
    out_ref[ROWS:BUF_ROWS] = total


def prep_body(
    ld_hbm, v_hbm, k_hbm, d_ref, toend_ref, total_ref, send_ref, mine_ref, k_ref,
    ld_ref, theirs_ref, sems,
):
    me = core_index()
    columns = lambda side: pl.ds(pl.multiple_of(side * ROWS, ROWS), ROWS)
    pairs = (
        (v_hbm.at[:, columns(1 - me)], theirs_ref), (ld_hbm, ld_ref), (k_hbm, k_ref),
        (v_hbm.at[:, columns(me)], mine_ref),
    )
    copies = [pltpu.make_async_copy(a, b, sems.at[i]) for i, (a, b) in enumerate(pairs)]
    for copy in copies:
        copy.start()
    row = lax.broadcasted_iota(jnp.int32, (128, 128), 0)
    col = lax.broadcasted_iota(jnp.int32, (128, 128), 1)
    upto = (row <= col).astype(F32).astype(BF16)
    copies[1].wait()
    terms = []
    for j in range(4):
        ld = ld_ref[:, j * 128 : (j + 1) * 128]
        terms += [*split3(ld), jnp.zeros_like(ld)]
    sums = jnp.dot(jnp.concatenate(terms, axis=0).astype(BF16), upto, preferred_element_type=F32)
    inner, totals = [], []
    for j in range(4):
        base = j * 32
        part = sums[base : base + 8] + sums[base + 8 : base + 16] + sums[base + 16 : base + 24]
        inner.append(part)
        totals.append(jnp.broadcast_to(part[:, 127:128], (HEADS, 128)))
    ahead = jnp.zeros((HEADS, 128), F32)
    d = []
    for j in range(4):
        d.append(inner[j] + ahead)
        ahead = ahead + totals[j]
    total = ahead
    total_ref[...] = total
    for j in range(4):
        cols = slice(j * 128, (j + 1) * 128)
        d_ref[:, cols] = d[j]
        toend_ref[:, cols] = jnp.exp(total - d[j])
    copies[0].wait()
    copies[2].wait()
    product(theirs_ref[...], toend_ref, total, 1 - me, k_ref[...], send_ref)
    copies[3].wait()


def prep(ld, v, k):
    outs = [sds((HEADS, BLOCK)), sds((HEADS, BLOCK)), sds((HEADS, 128)), sds((BUF_ROWS, STATE))]
    outs += [sds((BLOCK, ROWS), BF16), sds((BLOCK, STATE), BF16)]
    return call(
        prep_body, outs, [HB] * 3, 10**7,
        scratch=[
            pltpu.VMEM((HEADS, BLOCK), F32),
            pltpu.VMEM((BLOCK, ROWS), BF16),
            pltpu.SemaphoreType.DMA((4,)),
        ],
    )(*(pltpu.with_memory_space_constraint(x, pltpu.HBM) for x in (ld, v, k)))


def own_body(v_ref, k_ref, toend_ref, total_ref, out_ref):
    product(v_ref[...], toend_ref, total_ref[...], core_index(), k_ref[...], out_ref)


def own_state(v, k, toend, total):
    return call(own_body, sds((BUF_ROWS, STATE)), [VM] * 4, 10**6)(v, k, toend, total)


def merge_body(level, own_ref, got_ref, *refs):
    out_ref, fac_ref = refs[-2:]
    upper = ((lax.axis_index("tok") >> level) & 1) == 1
    own_ext = own_ref[ROWS:BUF_ROWS]
    got_ext = got_ref[ROWS:BUF_ROWS]
    one = jnp.ones_like(own_ext)
    fac_ref[0:HEADS] = jnp.where(upper, one, jnp.exp(got_ext))
    fac_ref[HEADS : 2 * HEADS] = jnp.where(upper, jnp.exp(own_ext), one)
    first = core_index() * HALF
    for j in range(HALF):
        rows = slice(j * WIDTH, (j + 1) * WIDTH)
        fa = fac_ref[pl.ds(first + j, 1), :]
        fb = fac_ref[pl.ds(first + (HEADS + j), 1), :]
        out_ref[rows] = own_ref[rows] * fa + got_ref[rows] * fb
    out_ref[ROWS:BUF_ROWS] = own_ext + got_ext


def merge(level, own, got, *tokens):
    return call(
        functools.partial(merge_body, level), sds((BUF_ROWS, STATE)),
        [VM] * (2 + len(tokens)), 10**5,
        scratch=[pltpu.VMEM((2 * HEADS, STATE), F32)], vmem=4,
    )(own, got, *tokens)


def aux_body(q_ref, gate_ref, d_ref, v_ref, qt_ref, gt_ref, dcol_ref, vt_ref):
    qt = q_ref[...].T
    qt_ref[0:STATE] = qt
    qt_ref[STATE : 2 * STATE] = qt
    vt_ref[...] = v_ref[...].T
    dcol_ref[...] = d_ref[...].T
    for j in range(4):
        cols = slice(j * 128, (j + 1) * 128)
        v = gate_ref[:, cols].T.astype(F32)
        gt_ref[cols] = v / (1.0 + jnp.exp(-v))


def aux(q, gate, d, v):
    outs = [sds((2 * STATE, BLOCK), BF16), sds((BLOCK, BLOCK)), sds((BLOCK, HEADS))]
    outs += [sds((BLOCK, BLOCK), BF16)]
    return call(aux_body, outs, [VM] * 4, 10**7)(q, gate, d, v)


def near_body(first, k_ref, qt_ref, vt_ref, d_ref, dcol_ref, w_ref, skip_ref, token_ref, out_ref, sc_ref, mix_ref):
    sc_ref[...] = jnp.dot(k_ref[...], qt_ref[0:STATE], preferred_element_type=F32)
    half = BLOCK // 2
    mix_ref[half:BLOCK, 0:half] = jnp.zeros((half, half), BF16)
    mix_ref[128:256, 0:128] = jnp.zeros((128, 128), BF16)
    mix_ref[384:512, 256:384] = jnp.zeros((128, 128), BF16)
    srow = lax.broadcasted_iota(jnp.int32, (128, 128), 0)
    tcol = lax.broadcasted_iota(jnp.int32, (128, 128), 1)
    cross = srow ^ tcol
    causal = srow <= tcol
    for n in range(2):
        h = first + n
        for i in range(4):
            rows = slice(i * 128, (i + 1) * 128)
            dcol = jnp.broadcast_to(dcol_ref[rows, h : h + 1], (128, 128))
            for j in range(i, 4):
                cols = slice(j * 128, (j + 1) * 128)
                spread = d_ref[h : h + 1, cols] - dcol
                if i == j:
                    spread = jnp.where(causal, spread, -jnp.inf)
                    chosen = jnp.broadcast_to(w_ref[0, h : h + 1, cols], (128, 128))
                    for level in range(1, 8):
                        chosen = jnp.where(
                            cross >= 1 << (level - 1), w_ref[level, h : h + 1, cols], chosen
                        )
                else:
                    chosen = w_ref[7 + (i ^ j).bit_length(), h : h + 1, cols]
                mix_ref[rows, cols] = (sc_ref[rows, cols] * jnp.exp(spread) * chosen).astype(BF16)
        mine = slice(h * WIDTH, (h + 1) * WIDTH)
        here = slice(n * WIDTH, (n + 1) * WIDTH)
        vt = vt_ref[mine]
        skip = vt.astype(F32) * skip_ref[h]
        out_ref[here, 0:half] = skip[:, 0:half] + jnp.dot(
            vt[:, 0:half], mix_ref[0:half, 0:half], preferred_element_type=F32
        )
        out_ref[here, half:BLOCK] = skip[:, half:BLOCK] + jnp.dot(
            vt, mix_ref[:, half:BLOCK], preferred_element_type=F32
        )


def near(first, k, qt, vt, d, dcol, w, skip, token):
    return call(
        functools.partial(near_body, first), sds((2 * WIDTH, BLOCK)), [VM] * 6 + [SM, VM],
        10**7,
        scratch=[pltpu.VMEM((BLOCK, BLOCK), F32), pltpu.VMEM((BLOCK, BLOCK), BF16)],
    )(k, qt, vt, d, dcol, w, skip, token)


def readout(level, sides, acc_rows, emit, qt_ref, d_ref, w_ref, lead, buf_refs, coef_ref):
    upper = ((lax.axis_index("tok") >> level) & 1) == 1
    gain = jnp.where(upper, jnp.exp(lead), 0.0)[:, 0:1]
    coef_ref[...] = w_ref[LOCAL_BITS + 1 + level] * jnp.exp(d_ref[...]) * gain
    core = core_index()
    for n, ref in zip(sides, buf_refs):
        side = core if n == 0 else 1 - core
        states = ref[0:ROWS]
        hi = states.astype(BF16)
        lo = (states - hi.astype(F32)).astype(BF16)
        read = jnp.dot(jnp.concatenate([hi, lo], axis=1), qt_ref[...], preferred_element_type=F32)
        for j in range(HALF):
            head = side * HALF + j
            row = pl.multiple_of(head * WIDTH, WIDTH)
            term = read[j * WIDTH : (j + 1) * WIDTH] * coef_ref[pl.ds(head, 1), :]
            emit(row, acc_rows(row) + term)


def far_body(level, qt_ref, d_ref, w_ref, lead_ref, *rest):
    coef_ref, next_ref, out_ref = rest[-1], rest[-2], rest[-3]
    bufs = rest[:2]

    def emit(row, value):
        out_ref[pl.ds(row, WIDTH), :] = value

    def start(row):
        return rest[2][pl.ds(row, WIDTH), :] if level > 0 else 0.0

    lead = lead_ref[...]
    readout(level, (0, 1), start, emit, qt_ref, d_ref, w_ref, lead, bufs, coef_ref)
    upper = ((lax.axis_index("tok") >> level) & 1) == 1
    next_ref[...] = lead + jnp.where(upper, bufs[0][ROWS:BUF_ROWS], 0.0)
    if level > 0:
        for n, ref in enumerate(rest[3:-3]):
            rows = slice((level - 1 + n) * 2 * WIDTH, (level + n) * 2 * WIDTH)
            out_ref[rows] = out_ref[rows] + ref[...]


def far(level, qt, d, w, lead, bufs, *more):
    return call(
        functools.partial(far_body, level), [sds((BLOCK, BLOCK)), sds((HEADS, STATE))],
        [VM] * (6 + len(more)), 10**7,
        aliases={6: 0} if more else None,
        scratch=[pltpu.VMEM((HEADS, BLOCK), F32)],
    )(qt, d, w, lead, *bufs, *more)


def close_body(
    level, side, qt_ref, d_ref, w_ref, lead_ref, acc_ref, gt_ref, near_ref, far_ref, *rest
):
    out_ref, sq_ref, coef_ref = rest[-3:]
    sums = [] if side == 0 else [rest[0][...]]
    half = core_index() if side == 0 else 1 - core_index()
    place = lambda row: pl.ds(pl.multiple_of(row - half * ROWS, WIDTH), WIDTH)

    def keep(row, value):
        out_ref[place(row), :] = value

    def emit(row, value):
        gated = value * gt_ref[pl.ds(row, WIDTH), :]
        out_ref[place(row), :] = gated
        sums.append(jnp.sum(gated * gated, axis=0, keepdims=True))

    lead = lead_ref[...]
    readout(
        level, (side,), lambda row: acc_ref[pl.ds(row, WIDTH), :], keep,
        qt_ref, d_ref, w_ref, lead, (near_ref,), coef_ref,
    )
    upper = ((lax.axis_index("tok") >> level) & 1) == 1
    lead = lead + jnp.where(upper, near_ref[ROWS:BUF_ROWS], 0.0)
    readout(
        level + 1, (side,), lambda row: out_ref[place(row), :], emit,
        qt_ref, d_ref, w_ref, lead, (far_ref,), coef_ref,
    )
    sq_ref[...] = sum(sums[1:], sums[0])


def close(level, side, qt, d, w, lead, acc, gt, *bufs):
    return call(
        functools.partial(close_body, level, side), [sds((ROWS, BLOCK)), sds((1, BLOCK))],
        [VM] * (6 + len(bufs)), 10**7,
        scratch=[pltpu.VMEM((HEADS, BLOCK), F32)],
    )(qt, d, w, lead, acc, gt, *bufs)


def turn_body(own_ref, other_ref, gain_ref, out_ref):
    core = core_index()
    for ref, side in ((own_ref, core), (other_ref, 1 - core)):
        cols = pl.ds(pl.multiple_of(side * ROWS, ROWS), ROWS)
        gain = gain_ref[:, cols]
        for j in range(4):
            rows = slice(j * 128, (j + 1) * 128)
            out_ref[rows, cols] = ref[:, rows].T * gain


def turn(own, other, gain):
    return call(turn_body, sds((BLOCK, BLOCK)), [VM] * 3, 10**7)(own, other, gain)


def finish_body(width, g_ref, a_ref, b_ref, c_ref, e_ref, out_hbm, out_ref, sems):
    total = a_ref[...] + b_ref[...] + c_ref[...] + e_ref[...]
    scale = lax.rsqrt(total / width + epsilon)
    copies = []
    for j in range(4):
        rows = slice(j * 128, (j + 1) * 128)
        column = jnp.broadcast_to(scale[:, rows], (128, 128)).T
        for i in range(4):
            cols = slice(i * 128, (i + 1) * 128)
            out_ref[rows, cols] = (g_ref[rows, cols] * column).astype(BF16)
        copies.append(pltpu.make_async_copy(out_ref.at[rows], out_hbm.at[rows], sems.at[j]))
        copies[-1].start()
    for copy in copies:
        copy.wait()


def finish(width, g, sums):
    return call(
        functools.partial(finish_body, width), sds((BLOCK, BLOCK), BF16), [VM] * 5,
        10**8, out_space=HB,
        scratch=[pltpu.VMEM((BLOCK, BLOCK), BF16), pltpu.SemaphoreType.DMA((4,))],
    )(g, *sums)


def hop(x, axis, flip):
    count = lax.axis_size(axis)
    return lax.ppermute(x, axis, [(i, i ^ flip) for i in range(count)])


CORE, Z1, Z3, Z7, X1, X2, X3 = 1, 2, 6, 14, 16, 32, 48


def work(head_inputs, state_keys, state_queries, log_decay, level_weight, skip_scale, gate_input, norm_gain):
    w = level_weight.transpose(2, 1, 0)
    d, toend, total, send, mine, keys = prep(log_decay.T, head_inputs, state_keys)
    swap = lambda x: hop(x, "tok", CORE)

    def close_by(first, token):
        return near(first, keys, qt, vt, d, dcol, w, skip_scale, token)

    def step(level, lead, bufs, *more):
        return far(level, qt, d, w, lead, bufs, *more)

    got = swap(send)
    own = own_state(mine, keys, toend, total)
    chip = merge(0, own, got)
    qt, gt, dcol, vt = aux(state_queries, gate_input, d, head_inputs)
    levels = [(got, swap(own))]
    parts = [close_by(0, chip)]
    z1 = hop(chip, "tok", Z1)
    pair = merge(1, chip, z1, parts[0])
    levels.append((z1, swap(z1)))
    parts.append(close_by(2, pair))
    acc, lead = step(0, jnp.zeros((HEADS, STATE), F32), levels[0])
    z3 = hop(pair, "tok", Z3)
    quad = merge(2, pair, z3, parts[1], acc)
    levels.append((z3, swap(z3)))
    parts.append(close_by(4, quad))
    acc, lead = step(1, lead, levels[1], acc, parts[0])
    z7 = hop(quad, "tok", Z7)
    acc, lead = step(2, lead, levels[2], acc, parts[1])
    line = merge(3, quad, z7, parts[2], acc)
    levels.append((z7, swap(z7)))
    parts.append(close_by(6, line))
    acc, lead = step(3, lead, levels[3], acc, parts[2], parts[3])
    x2 = hop(line, "tok", X2)
    x1 = hop(line, "tok", X1)
    x3 = hop(line, "tok", X3)
    beyond = merge(4, x2, x3, acc)
    other = swap(beyond)
    last = (qt, d, w, lead, acc, gt)
    near_half, part = close(4, 0, *last, x1, beyond)
    rest, squares = close(4, 1, *last, swap(x1), other, part)
    shares = [hop(squares, "head", 2), hop(squares, "head", 1), hop(squares, "head", 3)]
    turned = turn(near_half, rest, norm_gain[None])
    return finish(HEADS * WIDTH * lax.axis_size("head"), turned, [squares, *shares])


def solution(mesh):
    return jax.shard_map(
        work,
        mesh=mesh,
        in_specs=(
            P("tok", "head"),
            P("tok", None),
            P("tok", None),
            P("tok", "head"),
            P("tok", "head", None),
            P("head"),
            P("tok", "head"),
            P("head"),
        ),
        out_specs=P("tok", "head"),
        check_vma=False,
    )
```

```python
import functools

import jax
import jax.numpy as jnp
from jax import lax
from jax.experimental import pallas as pl
from jax.experimental.pallas import tpu as pltpu
from jax.sharding import PartitionSpec as P


epsilon = 1e-05
BLOCK = 512
HEADS = 8
WIDTH = 64
STATE = 128
HALF = HEADS // 2
ROWS = HALF * WIDTH
BUF_ROWS = ROWS + HEADS
LOCAL_BITS = 9
F32 = jnp.float32
BF16 = jnp.bfloat16
VM = pl.BlockSpec(memory_space=pltpu.VMEM)
SM = pl.BlockSpec(memory_space=pltpu.SMEM)
HB = pl.BlockSpec(memory_space=pltpu.HBM)
MIB = 1024 * 1024


def call(body, outs, ins, flops, aliases=None, scratch=(), vmem=12, out_space=VM):
    return pl.pallas_call(
        body,
        out_shape=outs,
        in_specs=ins,
        out_specs=jax.tree.map(lambda _: out_space, outs),
        scratch_shapes=list(scratch),
        input_output_aliases=aliases or {},
        cost_estimate=pl.CostEstimate(flops=flops, bytes_accessed=MIB, transcendentals=0),
        compiler_params=pltpu.CompilerParams(vmem_limit_bytes=vmem * MIB),
    )


def sds(shape, dtype=F32):
    return jax.ShapeDtypeStruct(shape, dtype)


def half_index():
    position = lax.axis_index("tok")
    return (position ^ (position >> 1) ^ (position >> 5)) & 1


def split3(x):
    hi = x.astype(BF16).astype(F32)
    rest = x - hi
    mid = rest.astype(BF16).astype(F32)
    return hi, mid, rest - mid


def product(v, toend_ref, total, side, keys, out_ref):
    vt = v.T
    scaled = [
        (vt[j * WIDTH : (j + 1) * WIDTH].astype(F32) * toend_ref[pl.ds(side * HALF + j, 1), :])
        .astype(BF16)
        for j in range(HALF)
    ]
    out_ref[0:ROWS] = jnp.dot(
        jnp.concatenate(scaled, axis=0), keys, preferred_element_type=F32
    )
    out_ref[ROWS:BUF_ROWS] = total


def prep_body(
    ld_hbm, v_hbm, k_hbm, d_ref, toend_ref, total_ref, send_ref, mine_ref, k_ref,
    ld_ref, theirs_ref, sems,
):
    me = half_index()
    columns = lambda side: pl.ds(pl.multiple_of(side * ROWS, ROWS), ROWS)
    pairs = (
        (ld_hbm, ld_ref), (v_hbm.at[:, columns(1 - me)], theirs_ref), (k_hbm, k_ref),
        (v_hbm.at[:, columns(me)], mine_ref),
    )
    copies = [pltpu.make_async_copy(a, b, sems.at[i]) for i, (a, b) in enumerate(pairs)]
    for copy in copies:
        copy.start()
    row = lax.broadcasted_iota(jnp.int32, (128, 128), 0)
    col = lax.broadcasted_iota(jnp.int32, (128, 128), 1)
    upto = (row <= col).astype(F32).astype(BF16)
    copies[0].wait()
    terms = []
    for j in range(4):
        ld = ld_ref[:, j * 128 : (j + 1) * 128]
        terms += [*split3(ld), jnp.zeros_like(ld)]
    sums = jnp.dot(jnp.concatenate(terms, axis=0).astype(BF16), upto, preferred_element_type=F32)
    inner, totals = [], []
    for j in range(4):
        base = j * 32
        part = sums[base : base + 8] + sums[base + 8 : base + 16] + sums[base + 16 : base + 24]
        inner.append(part)
        totals.append(jnp.broadcast_to(part[:, 127:128], (HEADS, 128)))
    ahead = jnp.zeros((HEADS, 128), F32)
    d = []
    for j in range(4):
        d.append(inner[j] + ahead)
        ahead = ahead + totals[j]
    total = ahead
    total_ref[...] = total
    for j in range(4):
        cols = slice(j * 128, (j + 1) * 128)
        d_ref[:, cols] = d[j]
        toend_ref[:, cols] = jnp.exp(total - d[j])
    copies[1].wait()
    copies[2].wait()
    product(theirs_ref[...], toend_ref, total, 1 - me, k_ref[...], send_ref)
    copies[3].wait()


def prep(ld, v, k):
    outs = [sds((HEADS, BLOCK)), sds((HEADS, BLOCK)), sds((HEADS, 128)), sds((BUF_ROWS, STATE))]
    outs += [sds((BLOCK, ROWS), BF16), sds((BLOCK, STATE), BF16)]
    return call(
        prep_body, outs, [HB] * 3, 10**7,
        scratch=[
            pltpu.VMEM((HEADS, BLOCK), F32),
            pltpu.VMEM((BLOCK, ROWS), BF16),
            pltpu.SemaphoreType.DMA((4,)),
        ],
    )(*(pltpu.with_memory_space_constraint(x, pltpu.HBM) for x in (ld, v, k)))


def own_body(v_ref, k_ref, toend_ref, total_ref, out_ref):
    product(v_ref[...], toend_ref, total_ref[...], half_index(), k_ref[...], out_ref)


def own_state(v, k, toend, total):
    return call(own_body, sds((BUF_ROWS, STATE)), [VM] * 4, 10**6)(v, k, toend, total)


def merge_body(level, own_ref, got_ref, *refs):
    out_ref, fac_ref = refs[-2:]
    upper = ((lax.axis_index("tok") >> level) & 1) == 1
    own_ext = own_ref[ROWS:BUF_ROWS]
    got_ext = got_ref[ROWS:BUF_ROWS]
    one = jnp.ones_like(own_ext)
    fac_ref[0:HEADS] = jnp.where(upper, one, jnp.exp(got_ext))
    fac_ref[HEADS : 2 * HEADS] = jnp.where(upper, jnp.exp(own_ext), one)
    first = half_index() * HALF
    for j in range(HALF):
        rows = slice(j * WIDTH, (j + 1) * WIDTH)
        fa = fac_ref[pl.ds(first + j, 1), :]
        fb = fac_ref[pl.ds(first + (HEADS + j), 1), :]
        out_ref[rows] = own_ref[rows] * fa + got_ref[rows] * fb
    out_ref[ROWS:BUF_ROWS] = own_ext + got_ext


def merge(level, own, got, *tokens):
    return call(
        functools.partial(merge_body, level), sds((BUF_ROWS, STATE)),
        [VM] * (2 + len(tokens)), 10**5,
        scratch=[pltpu.VMEM((2 * HEADS, STATE), F32)], vmem=4,
    )(own, got, *tokens)


def aux_body(q_ref, gate_ref, d_ref, v_ref, qt_ref, gt_ref, dcol_ref, vt_ref):
    qt = q_ref[...].T
    qt_ref[0:STATE] = qt
    qt_ref[STATE : 2 * STATE] = qt
    vt_ref[...] = v_ref[...].T
    dcol_ref[...] = d_ref[...].T
    for j in range(4):
        cols = slice(j * 128, (j + 1) * 128)
        v = gate_ref[:, cols].T.astype(F32)
        gt_ref[cols] = v / (1.0 + jnp.exp(-v))


def aux(q, gate, d, v):
    outs = [sds((2 * STATE, BLOCK), BF16), sds((BLOCK, BLOCK)), sds((BLOCK, HEADS))]
    outs += [sds((BLOCK, BLOCK), BF16)]
    return call(aux_body, outs, [VM] * 4, 10**7)(q, gate, d, v)


def near_body(first, k_ref, qt_ref, vt_ref, d_ref, dcol_ref, w_ref, skip_ref, token_ref, out_ref, sc_ref, mix_ref):
    sc_ref[...] = jnp.dot(k_ref[...], qt_ref[0:STATE], preferred_element_type=F32)
    half = BLOCK // 2
    mix_ref[half:BLOCK, 0:half] = jnp.zeros((half, half), BF16)
    mix_ref[128:256, 0:128] = jnp.zeros((128, 128), BF16)
    mix_ref[384:512, 256:384] = jnp.zeros((128, 128), BF16)
    srow = lax.broadcasted_iota(jnp.int32, (128, 128), 0)
    tcol = lax.broadcasted_iota(jnp.int32, (128, 128), 1)
    cross = srow ^ tcol
    causal = srow <= tcol
    for n in range(2):
        h = first + n
        for i in range(4):
            rows = slice(i * 128, (i + 1) * 128)
            dcol = jnp.broadcast_to(dcol_ref[rows, h : h + 1], (128, 128))
            for j in range(i, 4):
                cols = slice(j * 128, (j + 1) * 128)
                spread = d_ref[h : h + 1, cols] - dcol
                if i == j:
                    spread = jnp.where(causal, spread, -jnp.inf)
                    chosen = jnp.broadcast_to(w_ref[0, h : h + 1, cols], (128, 128))
                    for level in range(1, 8):
                        chosen = jnp.where(
                            cross >= 1 << (level - 1), w_ref[level, h : h + 1, cols], chosen
                        )
                else:
                    chosen = w_ref[7 + (i ^ j).bit_length(), h : h + 1, cols]
                mix_ref[rows, cols] = (sc_ref[rows, cols] * jnp.exp(spread) * chosen).astype(BF16)
        mine = slice(h * WIDTH, (h + 1) * WIDTH)
        here = slice(n * WIDTH, (n + 1) * WIDTH)
        vt = vt_ref[mine]
        skip = vt.astype(F32) * skip_ref[h]
        out_ref[here, 0:half] = skip[:, 0:half] + jnp.dot(
            vt[:, 0:half], mix_ref[0:half, 0:half], preferred_element_type=F32
        )
        out_ref[here, half:BLOCK] = skip[:, half:BLOCK] + jnp.dot(
            vt, mix_ref[:, half:BLOCK], preferred_element_type=F32
        )


def near(first, k, qt, vt, d, dcol, w, skip, token):
    return call(
        functools.partial(near_body, first), sds((2 * WIDTH, BLOCK)), [VM] * 6 + [SM, VM],
        10**7,
        scratch=[pltpu.VMEM((BLOCK, BLOCK), F32), pltpu.VMEM((BLOCK, BLOCK), BF16)],
    )(k, qt, vt, d, dcol, w, skip, token)


def readout(level, sides, acc_rows, emit, qt_ref, d_ref, w_ref, lead, buf_refs, coef_ref):
    upper = ((lax.axis_index("tok") >> level) & 1) == 1
    gain = jnp.where(upper, jnp.exp(lead), 0.0)[:, 0:1]
    coef_ref[...] = w_ref[LOCAL_BITS + 1 + level] * jnp.exp(d_ref[...]) * gain
    core = half_index()
    for n, ref in zip(sides, buf_refs):
        side = core if n == 0 else 1 - core
        states = ref[0:ROWS]
        hi = states.astype(BF16)
        lo = (states - hi.astype(F32)).astype(BF16)
        read = jnp.dot(jnp.concatenate([hi, lo], axis=1), qt_ref[...], preferred_element_type=F32)
        for j in range(HALF):
            head = side * HALF + j
            row = pl.multiple_of(head * WIDTH, WIDTH)
            term = read[j * WIDTH : (j + 1) * WIDTH] * coef_ref[pl.ds(head, 1), :]
            emit(row, acc_rows(row) + term)


def far_body(level, qt_ref, d_ref, w_ref, lead_ref, *rest):
    coef_ref, next_ref, out_ref = rest[-1], rest[-2], rest[-3]
    bufs = rest[:2]

    def emit(row, value):
        out_ref[pl.ds(row, WIDTH), :] = value

    def start(row):
        return rest[2][pl.ds(row, WIDTH), :] if level > 0 else 0.0

    lead = lead_ref[...]
    readout(level, (0, 1), start, emit, qt_ref, d_ref, w_ref, lead, bufs, coef_ref)
    upper = ((lax.axis_index("tok") >> level) & 1) == 1
    next_ref[...] = lead + jnp.where(upper, bufs[0][ROWS:BUF_ROWS], 0.0)
    if level > 0:
        for n, ref in enumerate(rest[3:-3]):
            rows = slice((level - 1 + n) * 2 * WIDTH, (level + n) * 2 * WIDTH)
            out_ref[rows] = out_ref[rows] + ref[...]


def far(level, qt, d, w, lead, bufs, *more):
    return call(
        functools.partial(far_body, level), [sds((BLOCK, BLOCK)), sds((HEADS, STATE))],
        [VM] * (6 + len(more)), 10**7,
        aliases={6: 0} if more else None,
        scratch=[pltpu.VMEM((HEADS, BLOCK), F32)],
    )(qt, d, w, lead, *bufs, *more)


def close_body(
    level, side, qt_ref, d_ref, w_ref, lead_ref, acc_ref, gt_ref, near_ref, far_ref, *rest
):
    out_ref, sq_ref, coef_ref = rest[-3:]
    sums = [] if side == 0 else [rest[0][...]]
    half = half_index() if side == 0 else 1 - half_index()
    place = lambda row: pl.ds(pl.multiple_of(row - half * ROWS, WIDTH), WIDTH)

    def keep(row, value):
        out_ref[place(row), :] = value

    def emit(row, value):
        gated = value * gt_ref[pl.ds(row, WIDTH), :]
        out_ref[place(row), :] = gated
        sums.append(jnp.sum(gated * gated, axis=0, keepdims=True))

    lead = lead_ref[...]
    readout(
        level, (side,), lambda row: acc_ref[pl.ds(row, WIDTH), :], keep,
        qt_ref, d_ref, w_ref, lead, (near_ref,), coef_ref,
    )
    upper = ((lax.axis_index("tok") >> level) & 1) == 1
    lead = lead + jnp.where(upper, near_ref[ROWS:BUF_ROWS], 0.0)
    readout(
        level + 1, (side,), lambda row: out_ref[place(row), :], emit,
        qt_ref, d_ref, w_ref, lead, (far_ref,), coef_ref,
    )
    sq_ref[...] = sum(sums[1:], sums[0])


def close(level, side, qt, d, w, lead, acc, gt, *bufs):
    return call(
        functools.partial(close_body, level, side), [sds((ROWS, BLOCK)), sds((1, BLOCK))],
        [VM] * (6 + len(bufs)), 10**7,
        scratch=[pltpu.VMEM((HEADS, BLOCK), F32)],
    )(qt, d, w, lead, acc, gt, *bufs)


def turn_body(own_ref, other_ref, gain_ref, out_ref):
    core = half_index()
    for ref, side in ((own_ref, core), (other_ref, 1 - core)):
        cols = pl.ds(pl.multiple_of(side * ROWS, ROWS), ROWS)
        gain = gain_ref[:, cols]
        for j in range(4):
            rows = slice(j * 128, (j + 1) * 128)
            out_ref[rows, cols] = ref[:, rows].T * gain


def turn(own, other, gain):
    return call(turn_body, sds((BLOCK, BLOCK)), [VM] * 3, 10**7)(own, other, gain)


def finish_body(width, g_ref, a_ref, b_ref, c_ref, e_ref, out_hbm, out_ref, sems):
    total = a_ref[...] + b_ref[...] + c_ref[...] + e_ref[...]
    scale = lax.rsqrt(total / width + epsilon)
    copies = []
    for j in range(4):
        rows = slice(j * 128, (j + 1) * 128)
        column = jnp.broadcast_to(scale[:, rows], (128, 128)).T
        for i in range(4):
            cols = slice(i * 128, (i + 1) * 128)
            out_ref[rows, cols] = (g_ref[rows, cols] * column).astype(BF16)
        copies.append(pltpu.make_async_copy(out_ref.at[rows], out_hbm.at[rows], sems.at[j]))
        copies[-1].start()
    for copy in copies:
        copy.wait()


def finish(width, g, sums):
    return call(
        functools.partial(finish_body, width), sds((BLOCK, BLOCK), BF16), [VM] * 5,
        10**8, out_space=HB,
        scratch=[pltpu.VMEM((BLOCK, BLOCK), BF16), pltpu.SemaphoreType.DMA((4,))],
    )(g, *sums)


def hop(x, axis, flip):
    count = lax.axis_size(axis)
    return lax.ppermute(x, axis, [(i, i ^ flip) for i in range(count)])


CORE, Z1, Z3, Z7, X1, X2, X3 = 1, 3, 7, 15, 16, 33, 49


def work(head_inputs, state_keys, state_queries, log_decay, level_weight, skip_scale, gate_input, norm_gain):
    w = level_weight.transpose(2, 1, 0)
    d, toend, total, send, mine, keys = prep(log_decay.T, head_inputs, state_keys)
    swap = lambda x: hop(x, "tok", CORE)

    def close_by(first, token):
        return near(first, keys, qt, vt, d, dcol, w, skip_scale, token)

    def step(level, lead, bufs, *more):
        return far(level, qt, d, w, lead, bufs, *more)

    got = swap(send)
    own = own_state(mine, keys, toend, total)
    chip = merge(0, own, got)
    qt, gt, dcol, vt = aux(state_queries, gate_input, d, head_inputs)
    levels = [(got, swap(own))]
    parts = [close_by(0, chip)]
    z1 = hop(chip, "tok", Z1)
    pair = merge(1, chip, z1, parts[0])
    levels.append((z1, swap(z1)))
    parts.append(close_by(2, pair))
    acc, lead = step(0, jnp.zeros((HEADS, STATE), F32), levels[0])
    z3 = hop(pair, "tok", Z3)
    quad = merge(2, pair, z3, parts[1], acc)
    levels.append((z3, swap(z3)))
    parts.append(close_by(4, quad))
    acc, lead = step(1, lead, levels[1], acc, parts[0])
    z7 = hop(quad, "tok", Z7)
    acc, lead = step(2, lead, levels[2], acc, parts[1])
    line = merge(3, quad, z7, parts[2], acc)
    levels.append((z7, swap(z7)))
    parts.append(close_by(6, line))
    acc, lead = step(3, lead, levels[3], acc, parts[2], parts[3])
    x2 = hop(line, "tok", X2)
    x1 = hop(line, "tok", X1)
    x3 = hop(line, "tok", X3)
    fourth = swap(x1)
    beyond = merge(4, x2, x3, acc)
    other = swap(beyond)
    last = (qt, d, w, lead, acc, gt)
    near_half, part = close(4, 0, *last, x1, beyond)
    rest, squares = close(4, 1, *last, fourth, other, part)
    shares = [hop(squares, "head", 2), hop(squares, "head", 1), hop(squares, "head", 3)]
    turned = turn(near_half, rest, norm_gain[None])
    return finish(HEADS * WIDTH * lax.axis_size("head"), turned, [squares, *shares])


def solution(mesh):
    return jax.shard_map(
        work,
        mesh=mesh,
        in_specs=(
            P("tok", "head"),
            P("tok", None),
            P("tok", None),
            P("tok", "head"),
            P("tok", "head", None),
            P("head"),
            P("tok", "head"),
            P("head"),
        ),
        out_specs=P("tok", "head"),
        check_vma=False,
    )
```

```python
import functools

import jax
import jax.numpy as jnp
from jax import lax
from jax.experimental import pallas as pl
from jax.experimental.pallas import tpu as pltpu
from jax.sharding import PartitionSpec as P


epsilon = 1e-05
BLOCK = 512
HEADS = 8
WIDTH = 64
STATE = 128
HALF = HEADS // 2
ROWS = HALF * WIDTH
BUF_ROWS = ROWS + HEADS
LOCAL_BITS = 9
F32 = jnp.float32
BF16 = jnp.bfloat16
VM = pl.BlockSpec(memory_space=pltpu.VMEM)
SM = pl.BlockSpec(memory_space=pltpu.SMEM)
HB = pl.BlockSpec(memory_space=pltpu.HBM)
MIB = 1024 * 1024


def call(body, outs, ins, flops, aliases=None, scratch=(), vmem=12, out_space=VM):
    return pl.pallas_call(
        body,
        out_shape=outs,
        in_specs=ins,
        out_specs=jax.tree.map(lambda _: out_space, outs),
        scratch_shapes=list(scratch),
        input_output_aliases=aliases or {},
        cost_estimate=pl.CostEstimate(flops=flops, bytes_accessed=MIB, transcendentals=0),
        compiler_params=pltpu.CompilerParams(vmem_limit_bytes=vmem * MIB),
    )


def sds(shape, dtype=F32):
    return jax.ShapeDtypeStruct(shape, dtype)


def core_index():
    return lax.axis_index("tok") & 1


def split3(x):
    hi = x.astype(BF16).astype(F32)
    rest = x - hi
    mid = rest.astype(BF16).astype(F32)
    return hi, mid, rest - mid


def product(v, toend_ref, total, side, keys, out_ref):
    vt = v.T
    scaled = [
        (vt[j * WIDTH : (j + 1) * WIDTH].astype(F32) * toend_ref[pl.ds(side * HALF + j, 1), :])
        .astype(BF16)
        for j in range(HALF)
    ]
    out_ref[0:ROWS] = jnp.dot(
        jnp.concatenate(scaled, axis=0), keys, preferred_element_type=F32
    )
    out_ref[ROWS:BUF_ROWS] = total


def prep_body(
    ld_hbm, v_hbm, k_hbm, d_ref, toend_ref, total_ref, send_ref, mine_ref, k_ref,
    ld_ref, theirs_ref, sems,
):
    me = core_index()
    columns = lambda side: pl.ds(pl.multiple_of(side * ROWS, ROWS), ROWS)
    pairs = (
        (ld_hbm, ld_ref), (v_hbm.at[:, columns(1 - me)], theirs_ref), (k_hbm, k_ref),
        (v_hbm.at[:, columns(me)], mine_ref),
    )
    copies = [pltpu.make_async_copy(a, b, sems.at[i]) for i, (a, b) in enumerate(pairs)]
    for copy in copies:
        copy.start()
    row = lax.broadcasted_iota(jnp.int32, (128, 128), 0)
    col = lax.broadcasted_iota(jnp.int32, (128, 128), 1)
    upto = (row <= col).astype(F32).astype(BF16)
    copies[0].wait()
    terms = []
    for j in range(4):
        ld = ld_ref[:, j * 128 : (j + 1) * 128]
        terms += [*split3(ld), jnp.zeros_like(ld)]
    sums = jnp.dot(jnp.concatenate(terms, axis=0).astype(BF16), upto, preferred_element_type=F32)
    inner, totals = [], []
    for j in range(4):
        base = j * 32
        part = sums[base : base + 8] + sums[base + 8 : base + 16] + sums[base + 16 : base + 24]
        inner.append(part)
        totals.append(jnp.broadcast_to(part[:, 127:128], (HEADS, 128)))
    ahead = jnp.zeros((HEADS, 128), F32)
    d = []
    for j in range(4):
        d.append(inner[j] + ahead)
        ahead = ahead + totals[j]
    total = ahead
    total_ref[...] = total
    for j in range(4):
        cols = slice(j * 128, (j + 1) * 128)
        d_ref[:, cols] = d[j]
        toend_ref[:, cols] = jnp.exp(total - d[j])
    copies[1].wait()
    copies[2].wait()
    product(theirs_ref[...], toend_ref, total, 1 - me, k_ref[...], send_ref)
    copies[3].wait()


def prep(ld, v, k):
    outs = [sds((HEADS, BLOCK)), sds((HEADS, BLOCK)), sds((HEADS, 128)), sds((BUF_ROWS, STATE))]
    outs += [sds((BLOCK, ROWS), BF16), sds((BLOCK, STATE), BF16)]
    return call(
        prep_body, outs, [HB] * 3, 10**7,
        scratch=[
            pltpu.VMEM((HEADS, BLOCK), F32),
            pltpu.VMEM((BLOCK, ROWS), BF16),
            pltpu.SemaphoreType.DMA((4,)),
        ],
    )(*(pltpu.with_memory_space_constraint(x, pltpu.HBM) for x in (ld, v, k)))


def own_body(v_ref, k_ref, toend_ref, total_ref, out_ref):
    product(v_ref[...], toend_ref, total_ref[...], core_index(), k_ref[...], out_ref)


def own_state(v, k, toend, total):
    return call(own_body, sds((BUF_ROWS, STATE)), [VM] * 4, 10**6)(v, k, toend, total)


def merge_body(level, own_ref, got_ref, *refs):
    out_ref, fac_ref = refs[-2:]
    upper = ((lax.axis_index("tok") >> level) & 1) == 1
    own_ext = own_ref[ROWS:BUF_ROWS]
    got_ext = got_ref[ROWS:BUF_ROWS]
    one = jnp.ones_like(own_ext)
    fac_ref[0:HEADS] = jnp.where(upper, one, jnp.exp(got_ext))
    fac_ref[HEADS : 2 * HEADS] = jnp.where(upper, jnp.exp(own_ext), one)
    first = core_index() * HALF
    for j in range(HALF):
        rows = slice(j * WIDTH, (j + 1) * WIDTH)
        fa = fac_ref[pl.ds(first + j, 1), :]
        fb = fac_ref[pl.ds(first + (HEADS + j), 1), :]
        out_ref[rows] = own_ref[rows] * fa + got_ref[rows] * fb
    out_ref[ROWS:BUF_ROWS] = own_ext + got_ext


def merge(level, own, got, *tokens):
    return call(
        functools.partial(merge_body, level), sds((BUF_ROWS, STATE)),
        [VM] * (2 + len(tokens)), 10**5,
        scratch=[pltpu.VMEM((2 * HEADS, STATE), F32)], vmem=4,
    )(own, got, *tokens)


def aux_body(q_ref, gate_ref, d_ref, v_ref, qt_ref, gt_ref, dcol_ref, vt_ref):
    qt = q_ref[...].T
    qt_ref[0:STATE] = qt
    qt_ref[STATE : 2 * STATE] = qt
    vt_ref[...] = v_ref[...].T
    dcol_ref[...] = d_ref[...].T
    for j in range(4):
        cols = slice(j * 128, (j + 1) * 128)
        v = gate_ref[:, cols].T.astype(F32)
        gt_ref[cols] = v / (1.0 + jnp.exp(-v))


def aux(q, gate, d, v):
    outs = [sds((2 * STATE, BLOCK), BF16), sds((BLOCK, BLOCK)), sds((BLOCK, HEADS))]
    outs += [sds((BLOCK, BLOCK), BF16)]
    return call(aux_body, outs, [VM] * 4, 10**7)(q, gate, d, v)


def near_body(first, k_ref, qt_ref, vt_ref, d_ref, dcol_ref, w_ref, skip_ref, token_ref, out_ref, sc_ref, mix_ref):
    sc_ref[...] = jnp.dot(k_ref[...], qt_ref[0:STATE], preferred_element_type=F32)
    half = BLOCK // 2
    mix_ref[half:BLOCK, 0:half] = jnp.zeros((half, half), BF16)
    mix_ref[128:256, 0:128] = jnp.zeros((128, 128), BF16)
    mix_ref[384:512, 256:384] = jnp.zeros((128, 128), BF16)
    srow = lax.broadcasted_iota(jnp.int32, (128, 128), 0)
    tcol = lax.broadcasted_iota(jnp.int32, (128, 128), 1)
    cross = srow ^ tcol
    causal = srow <= tcol
    for n in range(2):
        h = first + n
        for i in range(4):
            rows = slice(i * 128, (i + 1) * 128)
            dcol = jnp.broadcast_to(dcol_ref[rows, h : h + 1], (128, 128))
            for j in range(i, 4):
                cols = slice(j * 128, (j + 1) * 128)
                spread = d_ref[h : h + 1, cols] - dcol
                if i == j:
                    spread = jnp.where(causal, spread, -jnp.inf)
                    chosen = jnp.broadcast_to(w_ref[0, h : h + 1, cols], (128, 128))
                    for level in range(1, 8):
                        chosen = jnp.where(
                            cross >= 1 << (level - 1), w_ref[level, h : h + 1, cols], chosen
                        )
                else:
                    chosen = w_ref[7 + (i ^ j).bit_length(), h : h + 1, cols]
                mix_ref[rows, cols] = (sc_ref[rows, cols] * jnp.exp(spread) * chosen).astype(BF16)
        mine = slice(h * WIDTH, (h + 1) * WIDTH)
        here = slice(n * WIDTH, (n + 1) * WIDTH)
        vt = vt_ref[mine]
        skip = vt.astype(F32) * skip_ref[h]
        out_ref[here, 0:half] = skip[:, 0:half] + jnp.dot(
            vt[:, 0:half], mix_ref[0:half, 0:half], preferred_element_type=F32
        )
        out_ref[here, half:BLOCK] = skip[:, half:BLOCK] + jnp.dot(
            vt, mix_ref[:, half:BLOCK], preferred_element_type=F32
        )


def near(first, k, qt, vt, d, dcol, w, skip, token):
    return call(
        functools.partial(near_body, first), sds((2 * WIDTH, BLOCK)), [VM] * 6 + [SM, VM],
        10**7,
        scratch=[pltpu.VMEM((BLOCK, BLOCK), F32), pltpu.VMEM((BLOCK, BLOCK), BF16)],
    )(k, qt, vt, d, dcol, w, skip, token)


def readout(level, sides, acc_rows, emit, qt_ref, d_ref, w_ref, lead, buf_refs, coef_ref):
    upper = ((lax.axis_index("tok") >> level) & 1) == 1
    gain = jnp.where(upper, jnp.exp(lead), 0.0)[:, 0:1]
    coef_ref[...] = w_ref[LOCAL_BITS + 1 + level] * jnp.exp(d_ref[...]) * gain
    core = core_index()
    for n, ref in zip(sides, buf_refs):
        side = core if n == 0 else 1 - core
        states = ref[0:ROWS]
        hi = states.astype(BF16)
        lo = (states - hi.astype(F32)).astype(BF16)
        read = jnp.dot(jnp.concatenate([hi, lo], axis=1), qt_ref[...], preferred_element_type=F32)
        for j in range(HALF):
            head = side * HALF + j
            row = pl.multiple_of(head * WIDTH, WIDTH)
            term = read[j * WIDTH : (j + 1) * WIDTH] * coef_ref[pl.ds(head, 1), :]
            emit(row, acc_rows(row) + term)


def far_body(level, qt_ref, d_ref, w_ref, lead_ref, *rest):
    coef_ref, next_ref, out_ref = rest[-1], rest[-2], rest[-3]
    bufs = rest[:2]

    def emit(row, value):
        out_ref[pl.ds(row, WIDTH), :] = value

    def start(row):
        return rest[2][pl.ds(row, WIDTH), :] if level > 0 else 0.0

    lead = lead_ref[...]
    readout(level, (0, 1), start, emit, qt_ref, d_ref, w_ref, lead, bufs, coef_ref)
    upper = ((lax.axis_index("tok") >> level) & 1) == 1
    next_ref[...] = lead + jnp.where(upper, bufs[0][ROWS:BUF_ROWS], 0.0)
    if level > 0:
        for n, ref in enumerate(rest[3:-3]):
            rows = slice((level - 1 + n) * 2 * WIDTH, (level + n) * 2 * WIDTH)
            out_ref[rows] = out_ref[rows] + ref[...]


def far(level, qt, d, w, lead, bufs, *more):
    return call(
        functools.partial(far_body, level), [sds((BLOCK, BLOCK)), sds((HEADS, STATE))],
        [VM] * (6 + len(more)), 10**7,
        aliases={6: 0} if more else None,
        scratch=[pltpu.VMEM((HEADS, BLOCK), F32)],
    )(qt, d, w, lead, *bufs, *more)


def close_body(
    level, side, qt_ref, d_ref, w_ref, lead_ref, acc_ref, gt_ref, near_ref, far_ref, *rest
):
    out_ref, sq_ref, coef_ref = rest[-3:]
    sums = [] if side == 0 else [rest[0][...]]
    half = core_index() if side == 0 else 1 - core_index()
    place = lambda row: pl.ds(pl.multiple_of(row - half * ROWS, WIDTH), WIDTH)

    def keep(row, value):
        out_ref[place(row), :] = value

    def emit(row, value):
        gated = value * gt_ref[pl.ds(row, WIDTH), :]
        out_ref[place(row), :] = gated
        sums.append(jnp.sum(gated * gated, axis=0, keepdims=True))

    lead = lead_ref[...]
    readout(
        level, (side,), lambda row: acc_ref[pl.ds(row, WIDTH), :], keep,
        qt_ref, d_ref, w_ref, lead, (near_ref,), coef_ref,
    )
    upper = ((lax.axis_index("tok") >> level) & 1) == 1
    lead = lead + jnp.where(upper, near_ref[ROWS:BUF_ROWS], 0.0)
    readout(
        level + 1, (side,), lambda row: out_ref[place(row), :], emit,
        qt_ref, d_ref, w_ref, lead, (far_ref,), coef_ref,
    )
    sq_ref[...] = sum(sums[1:], sums[0])


def close(level, side, qt, d, w, lead, acc, gt, *bufs):
    return call(
        functools.partial(close_body, level, side), [sds((ROWS, BLOCK)), sds((1, BLOCK))],
        [VM] * (6 + len(bufs)), 10**7,
        scratch=[pltpu.VMEM((HEADS, BLOCK), F32)],
    )(qt, d, w, lead, acc, gt, *bufs)


def turn_body(own_ref, other_ref, gain_ref, out_ref):
    core = core_index()
    for ref, side in ((own_ref, core), (other_ref, 1 - core)):
        cols = pl.ds(pl.multiple_of(side * ROWS, ROWS), ROWS)
        gain = gain_ref[:, cols]
        for j in range(4):
            rows = slice(j * 128, (j + 1) * 128)
            out_ref[rows, cols] = ref[:, rows].T * gain


def turn(own, other, gain):
    return call(turn_body, sds((BLOCK, BLOCK)), [VM] * 3, 10**7)(own, other, gain)


def finish_body(width, g_ref, a_ref, b_ref, c_ref, e_ref, out_hbm, out_ref, sems):
    total = a_ref[...] + b_ref[...] + c_ref[...] + e_ref[...]
    scale = lax.rsqrt(total / width + epsilon)
    copies = []
    for j in range(4):
        rows = slice(j * 128, (j + 1) * 128)
        column = jnp.broadcast_to(scale[:, rows], (128, 128)).T
        for i in range(4):
            cols = slice(i * 128, (i + 1) * 128)
            out_ref[rows, cols] = (g_ref[rows, cols] * column).astype(BF16)
        copies.append(pltpu.make_async_copy(out_ref.at[rows], out_hbm.at[rows], sems.at[j]))
        copies[-1].start()
    for copy in copies:
        copy.wait()


def finish(width, g, sums):
    return call(
        functools.partial(finish_body, width), sds((BLOCK, BLOCK), BF16), [VM] * 5,
        10**8, out_space=HB,
        scratch=[pltpu.VMEM((BLOCK, BLOCK), BF16), pltpu.SemaphoreType.DMA((4,))],
    )(g, *sums)


def hop(x, axis, flip):
    count = lax.axis_size(axis)
    return lax.ppermute(x, axis, [(i, i ^ flip) for i in range(count)])


CORE, Z1, Z3, Z7, X1, X2, X3 = 1, 2, 6, 14, 16, 32, 48


def work(head_inputs, state_keys, state_queries, log_decay, level_weight, skip_scale, gate_input, norm_gain):
    w = level_weight.transpose(2, 1, 0)
    d, toend, total, send, mine, keys = prep(log_decay.T, head_inputs, state_keys)
    swap = lambda x: hop(x, "tok", CORE)

    def close_by(first, token):
        return near(first, keys, qt, vt, d, dcol, w, skip_scale, token)

    def step(level, lead, bufs, *more):
        return far(level, qt, d, w, lead, bufs, *more)

    got = swap(send)
    own = own_state(mine, keys, toend, total)
    chip = merge(0, own, got)
    qt, gt, dcol, vt = aux(state_queries, gate_input, d, head_inputs)
    levels = [(got, swap(own))]
    parts = [close_by(0, chip)]
    z1 = hop(chip, "tok", Z1)
    pair = merge(1, chip, z1, parts[0])
    levels.append((z1, swap(z1)))
    parts.append(close_by(2, pair))
    z3 = hop(pair, "tok", Z3)
    quad = merge(2, pair, z3, parts[1])
    levels.append((z3, swap(z3)))
    parts.append(close_by(4, quad))
    acc, lead = step(0, jnp.zeros((HEADS, STATE), F32), levels[0])
    acc, lead = step(1, lead, levels[1], acc, parts[0])
    z7 = hop(quad, "tok", Z7)
    acc, lead = step(2, lead, levels[2], acc, parts[1])
    line = merge(3, quad, z7, parts[2], acc)
    levels.append((z7, swap(z7)))
    parts.append(close_by(6, line))
    acc, lead = step(3, lead, levels[3], acc, parts[2], parts[3])
    x2 = hop(line, "tok", X2)
    x1 = hop(line, "tok", X1)
    x3 = hop(line, "tok", X3)
    fourth = swap(x1)
    beyond = merge(4, x2, x3, acc)
    other = swap(beyond)
    last = (qt, d, w, lead, acc, gt)
    near_half, part = close(4, 0, *last, x1, beyond)
    rest, squares = close(4, 1, *last, fourth, other, part)
    shares = [hop(squares, "head", 2), hop(squares, "head", 1), hop(squares, "head", 3)]
    turned = turn(near_half, rest, norm_gain[None])
    return finish(HEADS * WIDTH * lax.axis_size("head"), turned, [squares, *shares])


def solution(mesh):
    return jax.shard_map(
        work,
        mesh=mesh,
        in_specs=(
            P("tok", "head"),
            P("tok", None),
            P("tok", None),
            P("tok", "head"),
            P("tok", "head", None),
            P("head"),
            P("tok", "head"),
            P("head"),
        ),
        out_specs=P("tok", "head"),
        check_vma=False,
    )
```
